128 devices in a mesh: expert: 64 (over z, y, x_lo, core), dp: 2 (over x_hi).
Axes of the slice: x: 4 (x_hi: 2, x_lo: 2; x = x_hi * 2 + x_lo), y: 4, z: 4, core: 2. Of those that a mesh axis runs over, the one named last changes fastest.
Arguments:
- tokens: bfloat16 [16384, 2880], P(('expert', 'dp')), may hold values from -6 to 6
- cotangent: bfloat16 [16384, 2880], P(('expert', 'dp')), may hold values from -3 to 3
- expert_ids: int32 [16384, 4], P(('expert', 'dp')), may hold values from 0 to 63, as said below
- slots: int32 [16384, 4], P(('expert', 'dp')), may hold values from -1 to 5, as said below
- probs: float32 [16384, 4], P(('expert', 'dp')), may hold values from 0.1 to 0.6
- w_gate: bfloat16 [64, 2880, 1440], P('expert', None, 'dp'), may hold values from -0.109375 to 0.109375
- w_up: bfloat16 [64, 2880, 1440], P('expert', None, 'dp'), may hold values from -0.109375 to 0.109375
- w_down: bfloat16 [64, 2880, 1440], P('expert', None, 'dp'), may hold values from -0.15625 to 0.15625
Outputs:
- input_grad: bfloat16 [16384, 2880], P(('expert', 'dp'))
- prob_grad: float32 [16384, 4], P(('expert', 'dp'))
- grad_gate: bfloat16 [64, 2880, 1440], P('expert', None, 'dp')
- grad_up: bfloat16 [64, 2880, 1440], P('expert', None, 'dp')
- grad_down: bfloat16 [64, 2880, 1440], P('expert', None, 'dp')
The draws below stay inside these ranges and needn't reach their ends.
Inputs may be any that keep to these rules, and one draw needn't show every extreme that they name: `expert_ids`: each row names 4 different experts. Within the 128 tokens of one device, the choices of one expert, taken in order of tokens and then of k, hold 0, 1, 2 and so on up to 5, and -1 after that; in every draw some expert fills all 6 slots from every device.
All inputs are finite; a program needn't handle non-finite values.
Results may differ from the reference program's by a relative error of at most 0.018.
Values may be sent and summed in bfloat16 or wider, within the bound.
A program may use at most 192 MiB of HBM per device.

```python
import jax
import jax.numpy as jnp
from jax import lax

D = 2880
FFW = 1440
TOP = 4
TOK_DEV = 128
EXPERTS = 64
CAP = 6
TOKENS = 16384
N_EXPERT = 64
N_DP = 2


def routing_pair(key):
    base = jax.random.fold_in(key, 11)
    first_key, second_key, third_key = jax.random.split(base, 3)
    tokens_total = TOK_DEV * N_EXPERT * N_DP
    bias = jax.random.randint(first_key, (EXPERTS,), 0, 8192)
    hottest = jax.random.randint(second_key, (), 0, EXPERTS)
    expert_range = jnp.arange(EXPERTS, dtype=jnp.int32)
    bias = bias + jnp.where(expert_range == hottest, 40000, 0)
    scores = jax.random.randint(third_key, (tokens_total, EXPERTS), 0, 65536) + bias[None, :]
    scores = scores * EXPERTS + expert_range[None, :]
    ignored, chosen = lax.top_k(scores, TOP)
    chosen = chosen.astype(jnp.int32)
    onehot = (chosen[:, :, None] == expert_range[None, None, :]).astype(jnp.int32)
    onehot = onehot.reshape(tokens_total // TOK_DEV, TOK_DEV * TOP, EXPERTS)
    ranks = jnp.cumsum(onehot, axis=1) - 1
    ranks = jnp.sum(onehot * ranks, axis=2).reshape(tokens_total, TOP)
    slot_values = jnp.where(ranks < CAP, ranks, -1).astype(jnp.int32)
    return (chosen, slot_values)


def draw_expert_ids(key, part):
    chosen, slot_values = routing_pair(key)
    return chosen


def draw_slots(key, part):
    chosen, slot_values = routing_pair(key)
    return slot_values


def block_levels(stream_key, extent, cuts, low, top_value):
    loudness, own = 1.0, jax.random.fold_in(stream_key, 6)
    for dim, parts in cuts:
        steps = jnp.exp(jax.random.uniform(jax.random.fold_in(own, dim), (parts,), jnp.float32, low / len(cuts), top_value / len(cuts)))
        loudness = loudness * jnp.repeat(steps, extent[dim] // parts).reshape([-1 if axis == dim else 1 for axis in range(len(extent))])
    return loudness


def noise(rng, shape, width, most, cuts=(), held_as=jnp.bfloat16):
    drawn = width * jax.random.normal(rng, shape, jnp.float32)
    if cuts:
        drawn = drawn * block_levels(rng, shape, cuts, -0.22, 0.18)
    return jnp.clip(drawn, -most, most).astype(held_as)


def setup_inputs(seed: int = 0) -> dict:
    streams_of = jax.random.split(jax.random.key(seed), 9)
    return {
        "tokens": noise(streams_of[0], (TOKENS, D), 1.0, 6.0, ((0, 128),)),
        "cotangent": noise(streams_of[1], (TOKENS, D), 0.4, 3.0, ((0, 128),)),
        "expert_ids": draw_expert_ids(jax.random.fold_in(streams_of[8], 71), 0),
        "slots": draw_slots(jax.random.fold_in(streams_of[8], 71), 0),
        "probs": jnp.clip(0.1 + 0.5 * jax.random.uniform(streams_of[4], (TOKENS, TOP), jnp.float32) ** block_levels(streams_of[4], (TOKENS, TOP), ((0, 128),), -0.2, 0.2), 0.1, 0.6),
        "w_gate": noise(streams_of[5], (EXPERTS, D, FFW), D ** -0.5, 0.109375, ((0, 64), (2, 2))),
        "w_up": noise(streams_of[6], (EXPERTS, D, FFW), D ** -0.5, 0.109375, ((0, 64), (2, 2))),
        "w_down": noise(streams_of[7], (EXPERTS, D, FFW), FFW ** -0.5, 0.15625, ((0, 64), (2, 2))),
    }


ALPHA = 1.702


def reference(tokens, cotangent, expert_ids, slots, probs, w_gate, w_up, w_down):
    tokens_total = tokens.shape[0]
    blocks = tokens_total // TOK_DEV
    block_of = jnp.arange(tokens_total, dtype=jnp.int32) // TOK_DEV
    kept = slots >= 0
    position = jnp.where(kept, (expert_ids * blocks + block_of[:, None]) * CAP + slots, EXPERTS * blocks * CAP)
    owners = jnp.broadcast_to(jnp.arange(tokens_total, dtype=jnp.int32)[:, None], expert_ids.shape)
    slot_owner = jnp.full((EXPERTS * blocks * CAP,), -1, jnp.int32).at[position.reshape(-1)].set(owners.reshape(-1), mode="drop")
    slot_prob = jnp.zeros((EXPERTS * blocks * CAP,), jnp.float32).at[position.reshape(-1)].set(probs.reshape(-1), mode="drop")
    slot_owner = slot_owner.reshape(EXPERTS, blocks * CAP)
    slot_prob = slot_prob.reshape(EXPERTS, blocks * CAP)

    def expert_pass(operands):
        owner_col, prob_col, gate_w, up_w, down_w = operands
        present = owner_col >= 0
        source = jnp.maximum(owner_col, 0)
        rows = jnp.where(present[:, None], tokens[source], jnp.zeros((), jnp.bfloat16))
        gate_pre = jnp.dot(rows, gate_w, preferred_element_type=jnp.float32)
        up_pre = jnp.dot(rows, up_w, preferred_element_type=jnp.float32)
        sigmoid_val = jax.nn.sigmoid(ALPHA * gate_pre)
        glu_value = gate_pre * sigmoid_val
        hidden = ((up_pre + 1.0) * glu_value).astype(jnp.bfloat16)
        outputs = lax.dot_general(hidden, down_w, (((1,), (1,)), ((), ())), preferred_element_type=jnp.float32).astype(jnp.bfloat16)
        plain = jnp.where(present[:, None], cotangent[source], jnp.zeros((), jnp.bfloat16))
        slot_grad = jnp.sum(plain.astype(jnp.float32) * outputs.astype(jnp.float32), axis=1)
        weighted = (prob_col[:, None] * plain.astype(jnp.float32)).astype(jnp.bfloat16)
        hidden_grad = jnp.dot(weighted, down_w, preferred_element_type=jnp.float32)
        up_grad = (hidden_grad * glu_value).astype(jnp.bfloat16)
        gate_grad = (hidden_grad * (up_pre + 1.0) * (sigmoid_val + ALPHA * gate_pre * sigmoid_val * (1.0 - sigmoid_val))).astype(jnp.bfloat16)
        contract_rows = (((0,), (0,)), ((), ()))
        grad_down = lax.dot_general(weighted, hidden, contract_rows, preferred_element_type=jnp.float32).astype(jnp.bfloat16)
        grad_gate = lax.dot_general(rows, gate_grad, contract_rows, preferred_element_type=jnp.float32).astype(jnp.bfloat16)
        grad_up = lax.dot_general(rows, up_grad, contract_rows, preferred_element_type=jnp.float32).astype(jnp.bfloat16)
        contract_units = (((1,), (1,)), ((), ()))
        row_grad = lax.dot_general(gate_grad, gate_w, contract_units, preferred_element_type=jnp.float32)
        row_grad = row_grad + lax.dot_general(up_grad, up_w, contract_units, preferred_element_type=jnp.float32)
        return slot_grad, row_grad.astype(jnp.bfloat16), grad_gate, grad_up, grad_down

    slot_grads, row_grads, grad_gate, grad_up, grad_down = lax.map(expert_pass, (slot_owner, slot_prob, w_gate, w_up, w_down))
    lookup = jnp.where(kept, (expert_ids * blocks + block_of[:, None]) * CAP + slots, 0)
    prob_grad = jnp.where(kept, slot_grads.reshape(-1)[lookup], jnp.float32(0.0))
    flat_rows = row_grads.reshape(-1, tokens.shape[1])
    total = jnp.zeros(tokens.shape, jnp.float32)
    for choice_index in range(TOP):
        picked = flat_rows[lookup[:, choice_index]].astype(jnp.float32)
        total = total + jnp.where(kept[:, choice_index][:, None], picked, jnp.float32(0.0))
    input_grad = total.astype(jnp.bfloat16)
    return input_grad, prob_grad, grad_gate, grad_up, grad_down
```

```python
import functools

import jax
import jax.numpy as jnp
from jax import lax
from jax.experimental import pallas as pl
from jax.experimental.pallas import tpu as pltpu
from jax.sharding import PartitionSpec as P

ALPHA = 1.702
BF = jnp.bfloat16
F32 = jnp.float32
CAP = 6
MROWS = 8
MAIN = 2304
CHUNK = 640


def dot(a, b):
    return jnp.dot(a, b, preferred_element_type=F32)


def dot_nt(a, b):
    return lax.dot_general(a, b, (((1,), (1,)), ((), ())), preferred_element_type=F32)


def iota(shape, dim):
    return lax.broadcasted_iota(jnp.int32, shape, dim)


def pack_kernel(expert_ref, slot_ref, prob_ref, tok_ref, cot_ref, rows_ref, wt_ref, rem_ref):
    toks = tok_ref.shape[0]
    rest = tok_ref.shape[1] - MAIN
    total = rows_ref.shape[0]
    row = iota((total, toks), 0)
    zero = jnp.zeros((total, toks), F32)
    one, par, orem, prem = zero, zero, [zero] * 3, [zero] * 3
    for k in range(expert_ref.shape[0]):
        expert, slot, prob = expert_ref[k : k + 1, :], slot_ref[k : k + 1, :], prob_ref[k : k + 1, :]
        kept = slot >= 0
        hit = row == jnp.where(kept, expert * MROWS + slot, -1)
        one = jnp.where(hit, 1.0, one)
        par = jnp.where(hit, prob, par)
        high = jnp.where(slot >= 3, 1, 0)
        place = expert * MROWS + CAP + high
        for j in range(3):
            hit = row == jnp.where(kept & (slot - 3 * high == j), place, -1)
            orem[j] = jnp.where(hit, 1.0, orem[j])
            prem[j] = jnp.where(hit, prob, prem[j])
    rem_ref[...] = jnp.zeros_like(rem_ref)
    for src, dst, main, extra in ((tok_ref, rows_ref, one, orem), (cot_ref, wt_ref, par, prem)):
        rem_ref[:, :rest] = src[:, MAIN:]
        main = main.astype(BF)
        for j in range(3):
            cols = slice(j * CHUNK, (j + 1) * CHUNK)
            part = dot(main, src[:, cols]) + dot(extra[j].astype(BF), rem_ref[...])
            dst[:, cols] = part.astype(BF)
        cols = slice(3 * CHUNK, MAIN)
        dst[:, cols] = dot(main, src[:, cols]).astype(BF)


def pack(expert_t, slot_t, prob_t, tokens, cotangent, experts):
    shape = jax.ShapeDtypeStruct((experts * MROWS, MAIN), BF)
    return pl.pallas_call(
        pack_kernel,
        out_shape=(shape, shape),
        scratch_shapes=[pltpu.VMEM((tokens.shape[0], CHUNK), BF)],
        compiler_params=pltpu.CompilerParams(vmem_limit_bytes=40 * 2**20),
    )(expert_t, slot_t, prob_t, tokens, cotangent)


def picks(out_rows, in_rows, wide):
    if wide:
        q, o = iota((out_rows, in_rows), 0), iota((out_rows, in_rows), 1)
    else:
        o, q = iota((out_rows, in_rows), 0), iota((out_rows, in_rows), 1)
    message = o // CAP
    slot = o - CAP * message
    base = q - MROWS * message
    high = jnp.where(slot >= 3, 1, 0)
    main = jnp.where(base == slot, 1.0, 0.0).astype(BF)
    last = base == CAP + high
    rem = [jnp.where(last & (slot - 3 * high == j), 1.0, 0.0).astype(BF) for j in range(3)]
    return main, rem, jnp.where(last, 1.0, 0.0).astype(BF)


def unpack_into(src, dst):
    main, rem, _ = picks(dst.shape[0], src.shape[0], False)
    rest = dst.shape[1] - MAIN
    dst[:, :MAIN] = dot(main, src[:, :MAIN]).astype(BF)
    part = dot(rem[0], src[:, :rest])
    for j in (1, 2):
        part = part + dot(rem[j], src[:, j * CHUNK : j * CHUNK + rest])
    dst[:, MAIN:] = part.astype(BF)


def forward_kernel(msg_ref, gate_ref, up_ref, rows_ref, hidden_ref, glu_ref, slope_ref):
    unpack_into(msg_ref, rows_ref)
    gate = dot(rows_ref[...], gate_ref[...])
    up = dot(rows_ref[...], up_ref[...]) + 1.0
    sig = jax.nn.sigmoid(ALPHA * gate)
    glu = gate * sig
    hidden_ref[...] = (up * glu).astype(BF)
    glu_ref[...] = glu
    slope_ref[...] = up * (sig + ALPHA * glu * (1.0 - sig))


def forward(msgs, gate_w, up_w, tile):
    width, units = gate_w.shape
    groups = msgs.shape[0] // MROWS
    steps = groups * CAP // tile
    wide = tile // CAP * MROWS
    block = lambda cols: pl.BlockSpec((tile, cols), lambda i: (i, 0))
    whole = pl.BlockSpec((width, units), lambda i: (0, 0))
    rows = groups * CAP
    return pl.pallas_call(
        forward_kernel,
        grid=(steps,),
        in_specs=[pl.BlockSpec((wide, MAIN), lambda i: (i, 0)), whole, whole],
        out_specs=[block(width), block(units), block(units), block(units)],
        out_shape=[
            jax.ShapeDtypeStruct((rows, width), BF),
            jax.ShapeDtypeStruct((rows, units), BF),
            jax.ShapeDtypeStruct((rows, units), F32),
            jax.ShapeDtypeStruct((rows, units), F32),
        ],
        compiler_params=pltpu.CompilerParams(vmem_limit_bytes=60 * 2**20),
        cost_estimate=pl.CostEstimate(flops=4 * rows * width * units, bytes_accessed=20 * 2**20, transcendentals=0),
    )(msgs, gate_w, up_w)


def backward_kernel(
    msg_ref, gate_ref, up_ref, down_ref, hidden_ref, glu_ref, slope_ref, wt_ref, gg_ref, ug_ref, out_ref, full_ref
):
    tile = wt_ref.shape[0]
    width = wt_ref.shape[1]
    unpack_into(msg_ref, wt_ref)
    hgrad = dot(wt_ref[...], down_ref[...])
    share = jnp.sum(hgrad * hidden_ref[...].astype(F32), axis=1, keepdims=True)
    ug_ref[...] = (hgrad * glu_ref[...]).astype(BF)
    gg_ref[...] = (hgrad * slope_ref[...]).astype(BF)
    full_ref[:, width:] = jnp.zeros((tile, full_ref.shape[1] - width), BF)
    full_ref[:, :width] = (dot_nt(gg_ref[...], gate_ref[...]) + dot_nt(ug_ref[...], up_ref[...])).astype(BF)
    main, rem, last = picks(out_ref.shape[0], tile, True)
    tail = full_ref[:, MAIN : MAIN + CHUNK]
    for j in range(3):
        cols = slice(j * CHUNK, (j + 1) * CHUNK)
        out_ref[:, cols] = (dot(main, full_ref[:, cols]) + dot(rem[j], tail)).astype(BF)
    spare = MAIN - 3 * CHUNK
    lane = iota((tile, spare), 1)
    row = iota((tile, spare), 0)
    head = share.astype(BF).astype(F32)
    spot = 2 * ((row % CAP) % 3)
    pair = jnp.where(lane == spot, head, jnp.where(lane == spot + 1, share - head, 0.0)).astype(BF)
    cols = slice(3 * CHUNK, MAIN)
    out_ref[:, cols] = (dot(main, full_ref[:, cols]) + dot(last, pair)).astype(BF)


def backward(msgs, gate_w, up_w, down_w, hidden, glu, slope, tile):
    width, units = gate_w.shape
    rows = hidden.shape[0]
    wide = tile // CAP * MROWS
    block = lambda cols: pl.BlockSpec((tile, cols), lambda i: (i, 0))
    whole = pl.BlockSpec((width, units), lambda i: (0, 0))
    packed = pl.BlockSpec((wide, MAIN), lambda i: (i, 0))
    return pl.pallas_call(
        backward_kernel,
        grid=(rows // tile,),
        in_specs=[packed, whole, whole, whole, block(units), block(units), block(units)],
        out_specs=[block(width), block(units), block(units), packed],
        out_shape=[
            jax.ShapeDtypeStruct((rows, width), BF),
            jax.ShapeDtypeStruct((rows, units), BF),
            jax.ShapeDtypeStruct((rows, units), BF),
            jax.ShapeDtypeStruct(msgs.shape, BF),
        ],
        scratch_shapes=[pltpu.VMEM((tile, MAIN + CHUNK), BF)],
        compiler_params=pltpu.CompilerParams(vmem_limit_bytes=60 * 2**20),
        cost_estimate=pl.CostEstimate(flops=6 * rows * width * units, bytes_accessed=30 * 2**20, transcendentals=0),
    )(msgs, gate_w, up_w, down_w, hidden, glu, slope)


def combine_kernel(copies, expert_ref, slot_ref, prob_ref, back_ref, in_ref, prob_out_ref):
    toks, rest = in_ref.shape[0], in_ref.shape[1] - MAIN
    total = back_ref.shape[0]
    col = iota((toks, total), 1)
    message = col // MROWS
    place = col - message * MROWS
    holder = message // copies
    zero = jnp.zeros((toks, total), F32)
    main, rem = zero, [zero] * 3
    sums = []
    lane = iota((toks, 128), 1)
    shares = back_ref[:, 3 * CHUNK : 3 * CHUNK + 128]
    for k in range(expert_ref.shape[1]):
        expert, slot = expert_ref[:, k : k + 1], slot_ref[:, k : k + 1]
        kept = slot >= 0
        mine = holder == jnp.where(kept, expert, -1)
        high = jnp.where(slot >= 3, 1, 0)
        which = slot - 3 * high
        main = jnp.where(mine & (place == slot), 1.0, main)
        tail = mine & (place == CAP + high)
        for j in range(3):
            rem[j] = jnp.where(tail & (which == j), 1.0, rem[j])
        got = dot(jnp.where(tail, 1.0, 0.0).astype(BF), shares)
        got = jnp.where((lane == 2 * which) | (lane == 2 * which + 1), got, 0.0)
        sums.append(jnp.sum(got, axis=1, keepdims=True))
    in_ref[:, :MAIN] = dot(main.astype(BF), back_ref[...]).astype(BF)
    part = dot(rem[0].astype(BF), back_ref[:, :rest])
    for j in (1, 2):
        part = part + dot(rem[j].astype(BF), back_ref[:, j * CHUNK : j * CHUNK + rest])
    in_ref[:, MAIN:] = part.astype(BF)
    choice = iota(prob_ref.shape, 1)
    total_share = jnp.zeros(prob_ref.shape, F32)
    for k, value in enumerate(sums):
        total_share = jnp.where(choice == k, value, total_share)
    prob_out_ref[...] = jnp.where(slot_ref[...] >= 0, total_share / prob_ref[...], 0.0)


def combine(expert_ids, slots, probs, back, width, copies):
    return pl.pallas_call(
        functools.partial(combine_kernel, copies),
        out_shape=(
            jax.ShapeDtypeStruct((expert_ids.shape[0], width), BF),
            jax.ShapeDtypeStruct(probs.shape, F32),
        ),
        compiler_params=pltpu.CompilerParams(vmem_limit_bytes=40 * 2**20),
    )(expert_ids, slots, probs, back)


def body(tokens, cotangent, expert_ids, slots, probs, w_gate, w_up, w_down):
    experts = lax.axis_size("expert")
    copies = lax.axis_size("dp")
    devices = experts * copies
    width = tokens.shape[1]
    gate_w, up_w, down_w = w_gate[0], w_up[0], w_down[0]
    rounded = probs.astype(BF).astype(F32)
    rows_msg, wt_msg = pack(expert_ids.T, slots.T, rounded.T, tokens, cotangent, experts)

    def spread(msg):
        msg = jnp.broadcast_to(msg.reshape(experts, 1, MROWS, MAIN), (experts, copies, MROWS, MAIN))
        msg = msg.reshape(devices, MROWS, MAIN)
        return lax.all_to_all(msg, ("expert", "dp"), split_axis=0, concat_axis=0, tiled=True)

    rows_in = spread(rows_msg).reshape(devices * MROWS, MAIN)
    wt_in = spread(wt_msg).reshape(devices * MROWS, MAIN)
    rows, hidden, glu, slope = forward(rows_in, gate_w, up_w, 192)
    weighted, gate_grad, up_grad, packed = backward(wt_in, gate_w, up_w, down_w, hidden, glu, slope, 192)
    back = lax.all_to_all(
        packed.reshape(devices, MROWS, MAIN), ("expert", "dp"), split_axis=0, concat_axis=0, tiled=True
    ).reshape(devices * MROWS, MAIN)
    contract_rows = (((0,), (0,)), ((), ()))
    grad_down = lax.dot_general(weighted, hidden, contract_rows, preferred_element_type=F32).astype(BF)
    grad_gate = lax.dot_general(rows, gate_grad, contract_rows, preferred_element_type=F32).astype(BF)
    grad_up = lax.dot_general(rows, up_grad, contract_rows, preferred_element_type=F32).astype(BF)
    input_grad, prob_grad = combine(expert_ids, slots, rounded, back, width, copies)
    return input_grad, prob_grad, grad_gate[None], grad_up[None], grad_down[None]


def solution(mesh):
    token_spec = P(("expert", "dp"), None)
    weight_spec = P("expert", None, "dp")
    return jax.shard_map(
        body,
        mesh=mesh,
        in_specs=(token_spec,) * 5 + (weight_spec,) * 3,
        out_specs=(token_spec,) * 2 + (weight_spec,) * 3,
        check_vma=False,
    )
```

```python
import functools

import jax
import jax.numpy as jnp
from jax import lax
from jax.experimental import pallas as pl
from jax.experimental.pallas import tpu as pltpu
from jax.sharding import PartitionSpec as P

ALPHA = 1.702
BF = jnp.bfloat16
F32 = jnp.float32
CAP = 6
MROWS = 8
MAIN = 2304
CHUNK = 640


def dot(a, b):
    return jnp.dot(a, b, preferred_element_type=F32)


def dot_nt(a, b):
    return lax.dot_general(a, b, (((1,), (1,)), ((), ())), preferred_element_type=F32)


def iota(shape, dim):
    return lax.broadcasted_iota(jnp.int32, shape, dim)


def pack_kernel(code_ref, tok_ref, rows_ref, rem_ref):
    width, toks = tok_ref.shape
    total = rows_ref.shape[0]
    row = iota((total, 1), 0)
    slot = row % MROWS
    message = row // MROWS
    rem_ref[...] = jnp.zeros_like(rem_ref)
    rem_ref[: width - MAIN, :] = tok_ref[MAIN:, :]
    place_into(rows_ref, message, slot, [(code_ref[k : k + 1, :], None) for k in range(code_ref.shape[0])], tok_ref, rem_ref)


def place_into(dst, expert, slot, choices, src, rest):
    toks = src.shape[1]
    none = jnp.zeros((expert.shape[0], toks), F32)

    def matrix(wanted):
        out = none
        for code, prob in choices:
            out = jnp.where(code == wanted, 1.0 if prob is None else prob, out)
        return out.astype(BF)

    main = matrix(jnp.where(slot < CAP, expert * MROWS + slot, -2).astype(code_type(choices)))
    for j in range(3):
        cols = slice(j * CHUNK, (j + 1) * CHUNK)
        extra = matrix(jnp.where(slot >= CAP, expert * MROWS + 3 * (slot - CAP) + j, -2).astype(code_type(choices)))
        dst[:, cols] = (dot_nt(main, src[cols, :]) + dot_nt(extra, rest[...])).astype(BF)
    dst[:, 3 * CHUNK :] = dot_nt(main, src[3 * CHUNK : MAIN, :]).astype(BF)


def code_type(choices):
    return choices[0][0].dtype


def pack(code, tokens_t, experts):
    return pl.pallas_call(
        pack_kernel,
        out_shape=jax.ShapeDtypeStruct((experts * MROWS, MAIN), BF),
        scratch_shapes=[pltpu.VMEM((CHUNK, tokens_t.shape[1]), BF)],
        compiler_params=pltpu.CompilerParams(vmem_limit_bytes=40 * 2**20),
    )(code, tokens_t)


STEPS = (1, 3, 2)
LINE = ((1, 0), (3, 0), (2, 0), (1, 1), (3, 1), (2, 1), (0, 1))
MESH = pl.DeviceIdType.MESH
HALF = MAIN // 2
PARTS = 2
BLOCKS = 8 // PARTS


def exchange_kernel(table_ref, rows_ref, cot_ref, rows_out, wt_out, *scratch):
    (relay_a, held_a, relay_b, cots, tables, sent, rest, block_buf) = scratch[:8]
    (tab_s, tab_r, cot_s, cot_r, a1_s, a1_r, a2_s, a2_r, a3_s, a3_r, b1_s, b1_r, b2_s, b2_r, own) = scratch[8:]
    e, d = lax.axis_index("expert"), lax.axis_index("dp")
    z, y, x, c = e // 16, (e // 4) % 4, d * 2 + (e // 2) % 2, e % 2
    xc, sub = x * 2 + c, (x % 2) * 2 + c

    def device(dz, dy, dx=0, dc=0):
        ox = (x + dx) % 4
        return ((((z + dz) % 4) * 4 + (y + dy) % 4) * 2 + ox % 2) * 2 + (c + dc) % 2, ox // 2

    barrier = pltpu.get_barrier_semaphore()
    for step in STEPS:
        pl.semaphore_signal(barrier, inc=1, device_id=device(step, 0), device_id_type=MESH)
        pl.semaphore_signal(barrier, inc=1, device_id=device(0, step), device_id_type=MESH)
    for off in LINE:
        pl.semaphore_signal(barrier, inc=1, device_id=device(0, 0, *off), device_id_type=MESH)
    pl.semaphore_wait(barrier, 2 * len(STEPS) + len(LINE))

    started = []

    def send(src, dst, ssem, rsem, target):
        copy = pltpu.make_async_remote_copy(
            src_ref=src, dst_ref=dst, send_sem=ssem, recv_sem=rsem, device_id=target, device_id_type=MESH
        )
        copy.start()
        started.append(copy)
        return copy

    local = []

    def keep(src, dst, sem):
        copy = pltpu.make_async_copy(src, dst, sem)
        copy.start()
        local.append(copy)
        return copy

    mine = (z, y)
    halves = (pl.ds(0, HALF), pl.ds(HALF, HALF))

    def at(h, first, second):
        return (first, second) if h == 0 else (second, first)

    def first_step(h, step):
        return device(step, 0) if h == 0 else device(0, step)

    def second_step(h, step):
        return device(0, step) if h == 0 else device(step, 0)

    def pick(ref, h, first, second, *more):
        one, two = at(h, first, second)
        return ref.at[(one, two, *more)]

    every = slice(None)
    keep(cot_ref, cots.at[xc], own.at[0])
    keep(table_ref, tables.at[xc], own.at[1])
    a1 = [[None] * 3, [None] * 3]
    a2 = [[[None] * 3 for _ in range(4)] for _ in range(2)]
    for h in range(2):
        keep(rows_ref.at[z, y, :, :, halves[h]], relay_a.at[h, mine[h], mine[1 - h]], own.at[2 + h])
    for i, off in enumerate(LINE):
        tab = send(table_ref, tables.at[xc], tab_s.at[i], tab_r.at[i], device(0, 0, *off))
    tab_copies = started[-len(LINE) :]
    tail = cot_ref.shape[0] // 2
    parts = (pl.ds(0, tail), pl.ds(tail, tail))

    def send_cot(src, dst, k, target):
        return send(src, dst, cot_s.at[k], cot_r.at[k], target)

    near = [send_cot(cot_ref, cots.at[xc], i, device(0, 0, step)) for i, step in enumerate((1, 3))]
    for i, step in enumerate(STEPS):
        for h in range(2):
            to = (mine[h] + step) % 4
            a1[h][i] = send(
                pick(rows_ref, h, to, every, every, every, halves[h]),
                relay_a.at[h, mine[h]],
                a1_s.at[h, i],
                a1_r.at[h, i],
                first_step(h, step),
            )
    other_core = [send_cot(cot_ref, cots.at[xc], 4, device(0, 0, 0, 1))]

    def forward_rows(h, i, source):
        for j, step in enumerate(STEPS):
            to = (mine[1 - h] + step) % 4
            if source is None:
                src = pick(rows_ref, h, mine[h], to, every, every, halves[h])
                place = mine[h]
            else:
                src = relay_a.at[h, source, to]
                place = source
            a2[h][i][j] = send(src, held_a.at[h, mine[1 - h], place], a2_s.at[h, i, j], a2_r.at[h, i, j], second_step(h, step))

    for h in range(2):
        forward_rows(h, 3, None)
    def forward_a1(i):
        for h in range(2):
            a1[h][i].wait_recv()
            forward_rows(h, i, (mine[h] - STEPS[i]) % 4)

    forward_a1(0)
    forward_a1(1)
    far = []
    for i, step in enumerate((1, 3)):
        block = ((x - step) % 4) * 2 + c
        near[i].wait_recv()
        far.append(send_cot(cots.at[block, parts[i]], cots.at[block, parts[i]], 2 + i, device(0, 0, step)))
        other_core.append(send_cot(cots.at[block], cots.at[block], 5 + i, device(0, 0, 0, 1)))
    forward_a1(2)
    block = ((x + 2) % 4) * 2 + c
    for i in range(2):
        far[i].wait_recv()
        other_core.append(send_cot(cots.at[block, parts[i]], cots.at[block, parts[i]], 7 + i, device(0, 0, 0, 1)))

    def spread_rows(h, group, source, place):
        where = pick(rows_out, h, every, place, xc, every, halves[h])
        for k, off in enumerate(LINE):
            ox, oc = (x + off[0]) % 4, (c + off[1]) % 2
            send(
                source.at[:, (ox % 2) * 2 + oc],
                where,
                a3_s.at[h, group, k],
                a3_r.at[h, group, k],
                device(0, 0, *off),
            )
        keep(source.at[:, sub], where, own.at[4 + 4 * h + group])

    for copy in local[:4]:
        copy.wait()
    for h in range(2):
        spread_rows(h, 3, relay_a.at[h, :, mine[1 - h]], mine[1 - h])

    rest[...] = jnp.zeros_like(rest)
    width = cot_ref.shape[0]
    row = iota((16 * MROWS, 1), 0)

    def make_block(b):
        rest[: width - MAIN, :] = cots[b, MAIN:, :]
        choices = [(tables[b, k : k + 1, :], tables[b, 4 + k : 5 + k, :]) for k in range(4)]
        place_into(block_buf, (row // MROWS) * 4 + sub, row % MROWS, choices, cots.at[b], rest)
        sent[:, :, b] = block_buf[...].reshape(4, 4, MROWS, MAIN)

    for copy in tab_copies + other_core:
        copy.wait_recv()
    b1 = [[[None] * 3, [None] * 3] for _ in range(PARTS)]
    b2 = [[[[None] * 3 for _ in range(4)] for _ in range(2)] for _ in range(PARTS)]

    def forward_wts(p, h, i, source):
        blocks = pl.ds(p * BLOCKS, BLOCKS)
        for j, step in enumerate(STEPS + (0,)):
            to = (mine[1 - h] + step) % 4
            if source is None:
                src = pick(sent, h, mine[h], to, blocks, every, halves[h])
                place = mine[h]
            else:
                src = relay_b.at[h, source, to, blocks]
                place = source
            dst = pick(wt_out, h, place, mine[1 - h], blocks, every, halves[h])
            if step:
                b2[p][h][i][j] = send(src, dst, b2_s.at[p, h, i, j], b2_r.at[p, h, i, j], second_step(h, step))
            else:
                keep(src, dst, own.at[12 + (p * 2 + h) * 4 + i])

    for p in range(PARTS):
        blocks = pl.ds(p * BLOCKS, BLOCKS)

        @pl.loop(p * BLOCKS, (p + 1) * BLOCKS)
        def _(b):
            make_block(b)

        for i, step in enumerate(STEPS):
            for h in range(2):
                to = (mine[h] + step) % 4
                b1[p][h][i] = send(
                    pick(sent, h, to, every, blocks, every, halves[h]),
                    relay_b.at[h, mine[h], :, blocks],
                    b1_s.at[p, h, i],
                    b1_r.at[p, h, i],
                    first_step(h, step),
                )
        for h in range(2):
            forward_wts(p, h, 3, None)

    for j, step in enumerate(STEPS):
        for h in range(2):
            for i in range(4):
                a2[h][i][j].wait_recv()
            place = (mine[1 - h] - step) % 4
            spread_rows(h, j, held_a.at[h, place], place)

    for p in range(PARTS):
        for i, step in enumerate(STEPS):
            for h in range(2):
                b1[p][h][i].wait_recv()
                forward_wts(p, h, i, (mine[h] - step) % 4)

    early = {id(copy) for copy in tab_copies + near + far + other_core}
    for group in a1 + [v for half in a2 for v in half] + [v for part in b1 for v in part]:
        early |= {id(copy) for copy in group}
    for copy in local[4:]:
        copy.wait()
    for copy in started:
        if id(copy) not in early:
            copy.wait_recv()
    for copy in started:
        copy.wait_send()


def exchange(table, rows_msg, cot_t):
    out = jax.ShapeDtypeStruct((4, 4, 8, MROWS, MAIN), BF)
    anywhere = pl.BlockSpec(memory_space=pl.ANY)
    shapes = [(7,), (9,), (2, 3), (2, 4, 3), (2, 4, 7), (PARTS, 2, 3), (PARTS, 2, 4, 3)]
    sems = [pltpu.SemaphoreType.DMA(shape) for shape in shapes for _ in range(2)]
    return pl.pallas_call(
        exchange_kernel,
        in_specs=[anywhere] * 3,
        out_specs=[anywhere] * 2,
        out_shape=[out, out],
        scratch_shapes=[
            pltpu.VMEM((2, 4, 4, 4, MROWS, HALF), BF),
            pltpu.VMEM((2, 4, 4, 4, MROWS, HALF), BF),
            pltpu.VMEM((2, 4, 4, 8, MROWS, HALF), BF),
            pltpu.VMEM((8, *cot_t.shape), BF),
            pltpu.VMEM((8, *table.shape), F32),
            pltpu.VMEM((4, 4, 8, MROWS, MAIN), BF),
            pltpu.VMEM((CHUNK, cot_t.shape[1]), BF),
            pltpu.VMEM((16 * MROWS, MAIN), BF),
            *sems,
            pltpu.SemaphoreType.DMA((12 + 8 * PARTS,)),
        ],
        compiler_params=pltpu.CompilerParams(collective_id=0, has_side_effects=True, vmem_limit_bytes=48 * 2**20),
    )(table, rows_msg.reshape(4, 4, 4, MROWS, MAIN), cot_t)


def picks(out_rows, in_rows, wide, reorder=False):
    if wide:
        q, o = iota((out_rows, in_rows), 0), iota((out_rows, in_rows), 1)
    else:
        o, q = iota((out_rows, in_rows), 0), iota((out_rows, in_rows), 1)
    message = o // CAP
    slot = o - CAP * message
    if reorder:
        at = message % 8
        base = q - MROWS * (message - at + (at % 4) * 2 + at // 4)
    else:
        base = q - MROWS * message
    high = jnp.where(slot >= 3, 1, 0)
    main = jnp.where(base == slot, 1.0, 0.0).astype(BF)
    last = base == CAP + high
    rem = [jnp.where(last & (slot - 3 * high == j), 1.0, 0.0).astype(BF) for j in range(3)]
    return main, rem, jnp.where(last, 1.0, 0.0).astype(BF)


def unpack_into(src, dst):
    main, rem, _ = picks(dst.shape[0], src.shape[0], False)
    rest = dst.shape[1] - MAIN
    dst[:, :MAIN] = dot(main, src[:, :MAIN]).astype(BF)
    part = dot(rem[0], src[:, :rest])
    for j in (1, 2):
        part = part + dot(rem[j], src[:, j * CHUNK : j * CHUNK + rest])
    dst[:, MAIN:] = part.astype(BF)


def forward_kernel(msg_ref, gate_ref, up_ref, rows_ref, hidden_ref, glu_ref, slope_ref):
    unpack_into(msg_ref, rows_ref)
    gate = dot_nt(rows_ref[...], gate_ref[...])
    up = dot_nt(rows_ref[...], up_ref[...]) + 1.0
    sig = jax.nn.sigmoid(ALPHA * gate)
    glu = gate * sig
    hidden_ref[...] = (up * glu).astype(BF)
    glu_ref[...] = glu
    slope_ref[...] = up * (sig + ALPHA * glu * (1.0 - sig))


def forward(msgs, gate_w, up_w, tile):
    units, width = gate_w.shape
    groups = msgs.shape[0] // MROWS
    steps = groups * CAP // tile
    wide = tile // CAP * MROWS
    block = lambda cols: pl.BlockSpec((tile, cols), lambda i: (i, 0))
    whole = pl.BlockSpec((units, width), lambda i: (0, 0))
    rows = groups * CAP
    return pl.pallas_call(
        forward_kernel,
        grid=(steps,),
        in_specs=[pl.BlockSpec((wide, MAIN), lambda i: (i, 0)), whole, whole],
        out_specs=[block(width), block(units), block(units), block(units)],
        out_shape=[
            jax.ShapeDtypeStruct((rows, width), BF),
            jax.ShapeDtypeStruct((rows, units), BF),
            jax.ShapeDtypeStruct((rows, units), F32),
            jax.ShapeDtypeStruct((rows, units), F32),
        ],
        compiler_params=pltpu.CompilerParams(vmem_limit_bytes=60 * 2**20),
        cost_estimate=pl.CostEstimate(flops=4 * rows * width * units, bytes_accessed=20 * 2**20, transcendentals=0),
    )(msgs, gate_w, up_w)


def backward_kernel(
    msg_ref, gate_ref, up_ref, down_ref, hidden_ref, glu_ref, slope_ref, wt_ref, gg_ref, ug_ref, out_ref, full_ref
):
    tile = wt_ref.shape[0]
    width = wt_ref.shape[1]
    unpack_into(msg_ref, wt_ref)
    hgrad = dot_nt(wt_ref[...], down_ref[...])
    share = jnp.sum(hgrad * hidden_ref[...].astype(F32), axis=1, keepdims=True)
    ug_ref[...] = (hgrad * glu_ref[...]).astype(BF)
    gg_ref[...] = (hgrad * slope_ref[...]).astype(BF)
    full_ref[:, width:] = jnp.zeros((tile, full_ref.shape[1] - width), BF)
    full_ref[:, :width] = (dot(gg_ref[...], gate_ref[...]) + dot(ug_ref[...], up_ref[...])).astype(BF)
    main, rem, last = picks(out_ref.shape[0], tile, True, True)
    tail = full_ref[:, MAIN : MAIN + CHUNK]
    for j in range(3):
        cols = slice(j * CHUNK, (j + 1) * CHUNK)
        out_ref[:, cols] = (dot(main, full_ref[:, cols]) + dot(rem[j], tail)).astype(BF)
    spare = MAIN - 3 * CHUNK
    lane = iota((tile, spare), 1)
    row = iota((tile, spare), 0)
    head = share.astype(BF).astype(F32)
    spot = 2 * ((row % CAP) % 3)
    pair = jnp.where(lane == spot, head, jnp.where(lane == spot + 1, share - head, 0.0)).astype(BF)
    cols = slice(3 * CHUNK, MAIN)
    out_ref[:, cols] = (dot(main, full_ref[:, cols]) + dot(last, pair)).astype(BF)


def backward(msgs, gate_w, up_w, down_w, hidden, glu, slope, tile):
    units, width = gate_w.shape
    rows = hidden.shape[0]
    wide = tile // CAP * MROWS
    block = lambda cols: pl.BlockSpec((tile, cols), lambda i: (i, 0))
    whole = pl.BlockSpec((units, width), lambda i: (0, 0))
    packed = pl.BlockSpec((wide, MAIN), lambda i: (i, 0))
    return pl.pallas_call(
        backward_kernel,
        grid=(rows // tile,),
        in_specs=[packed, whole, whole, whole, block(units), block(units), block(units)],
        out_specs=[block(width), block(units), block(units), packed],
        out_shape=[
            jax.ShapeDtypeStruct((rows, width), BF),
            jax.ShapeDtypeStruct((rows, units), BF),
            jax.ShapeDtypeStruct((rows, units), BF),
            jax.ShapeDtypeStruct(msgs.shape, BF),
        ],
        scratch_shapes=[pltpu.VMEM((tile, MAIN + CHUNK), BF)],
        compiler_params=pltpu.CompilerParams(vmem_limit_bytes=60 * 2**20),
        cost_estimate=pl.CostEstimate(flops=6 * rows * width * units, bytes_accessed=30 * 2**20, transcendentals=0),
    )(msgs, gate_w, up_w, down_w, hidden, glu, slope)


def combine_kernel(copies, expert_ref, slot_ref, prob_ref, back_ref, in_ref, prob_out_ref):
    toks, rest = in_ref.shape[0], in_ref.shape[1] - MAIN
    total = back_ref.shape[0]
    col = iota((toks, total), 1)
    message = col // MROWS
    place = col - message * MROWS
    holder = message // copies
    zero = jnp.zeros((toks, total), F32)
    main, rem = zero, [zero] * 3
    sums = []
    lane = iota((toks, 128), 1)
    shares = back_ref[:, 3 * CHUNK : 3 * CHUNK + 128]
    for k in range(expert_ref.shape[1]):
        expert, slot = expert_ref[:, k : k + 1], slot_ref[:, k : k + 1]
        kept = slot >= 0
        mine = holder == jnp.where(kept, expert, -1)
        high = jnp.where(slot >= 3, 1, 0)
        which = slot - 3 * high
        main = jnp.where(mine & (place == slot), 1.0, main)
        tail = mine & (place == CAP + high)
        for j in range(3):
            rem[j] = jnp.where(tail & (which == j), 1.0, rem[j])
        got = dot(jnp.where(tail, 1.0, 0.0).astype(BF), shares)
        got = jnp.where((lane == 2 * which) | (lane == 2 * which + 1), got, 0.0)
        sums.append(jnp.sum(got, axis=1, keepdims=True))
    in_ref[:, :MAIN] = dot(main.astype(BF), back_ref[...]).astype(BF)
    part = dot(rem[0].astype(BF), back_ref[:, :rest])
    for j in (1, 2):
        part = part + dot(rem[j].astype(BF), back_ref[:, j * CHUNK : j * CHUNK + rest])
    in_ref[:, MAIN:] = part.astype(BF)
    choice = iota(prob_ref.shape, 1)
    total_share = jnp.zeros(prob_ref.shape, F32)
    for k, value in enumerate(sums):
        total_share = jnp.where(choice == k, value, total_share)
    prob_out_ref[...] = jnp.where(slot_ref[...] >= 0, total_share / prob_ref[...], 0.0)


def combine(expert_ids, slots, probs, back, width, copies):
    return pl.pallas_call(
        functools.partial(combine_kernel, copies),
        out_shape=(
            jax.ShapeDtypeStruct((expert_ids.shape[0], width), BF),
            jax.ShapeDtypeStruct(probs.shape, F32),
        ),
        compiler_params=pltpu.CompilerParams(vmem_limit_bytes=40 * 2**20),
    )(expert_ids, slots, probs, back)


def body(tokens, cotangent, expert_ids, slots, probs, w_gate, w_up, w_down):
    experts = lax.axis_size("expert")
    copies = lax.axis_size("dp")
    devices = experts * copies
    width = tokens.shape[1]
    gate_w, up_w, down_w = w_gate[0].T, w_up[0].T, w_down[0].T
    rounded = probs.astype(BF).astype(F32)
    code = jnp.where(slots >= 0, expert_ids * MROWS + slots, -1).T
    rows_msg = pack(code, tokens.T, experts)
    table = jnp.concatenate([code.astype(F32), rounded.T], axis=0)
    rows_in, wt_in = exchange(table, rows_msg, cotangent.T)
    rows_in = rows_in.reshape(devices * MROWS, MAIN)
    wt_in = wt_in.reshape(devices * MROWS, MAIN)
    rows, hidden, glu, slope = forward(rows_in, gate_w, up_w, 192)
    weighted, gate_grad, up_grad, packed = backward(wt_in, gate_w, up_w, down_w, hidden, glu, slope, 192)
    back = lax.all_to_all(
        packed.reshape(devices, MROWS, MAIN), ("expert", "dp"), split_axis=0, concat_axis=0, tiled=True
    ).reshape(devices * MROWS, MAIN)
    contract_rows = (((0,), (0,)), ((), ()))
    grad_down = lax.dot_general(weighted, hidden, contract_rows, preferred_element_type=F32).astype(BF)
    grad_gate = lax.dot_general(rows, gate_grad, contract_rows, preferred_element_type=F32).astype(BF)
    grad_up = lax.dot_general(rows, up_grad, contract_rows, preferred_element_type=F32).astype(BF)
    input_grad, prob_grad = combine(expert_ids, slots, rounded, back, width, copies)
    return input_grad, prob_grad, grad_gate[None], grad_up[None], grad_down[None]


def solution(mesh):
    token_spec = P(("expert", "dp"), None)
    weight_spec = P("expert", None, "dp")
    return jax.shard_map(
        body,
        mesh=mesh,
        in_specs=(token_spec,) * 5 + (weight_spec,) * 3,
        out_specs=(token_spec,) * 2 + (weight_spec,) * 3,
        check_vma=False,
    )
```

```python
import functools

import jax
import jax.numpy as jnp
from jax import lax
from jax.experimental import pallas as pl
from jax.experimental.pallas import tpu as pltpu
from jax.sharding import PartitionSpec as P

ALPHA = 1.702
BF = jnp.bfloat16
F32 = jnp.float32
CAP = 6
MROWS = 8
MAIN = 2304
CHUNK = 640


def dot(a, b):
    return jnp.dot(a, b, preferred_element_type=F32)


def dot_nt(a, b):
    return lax.dot_general(a, b, (((1,), (1,)), ((), ())), preferred_element_type=F32)


def iota(shape, dim):
    return lax.broadcasted_iota(jnp.int32, shape, dim)


def pack_kernel(code_ref, tok_ref, rows_ref, rem_ref):
    width, toks = tok_ref.shape
    total = rows_ref.shape[0]
    row = iota((total, 1), 0)
    slot = row % MROWS
    message = row // MROWS
    rem_ref[...] = jnp.zeros_like(rem_ref)
    rem_ref[: width - MAIN, :] = tok_ref[MAIN:, :]
    place_into(rows_ref, message, slot, [(code_ref[k : k + 1, :], None) for k in range(code_ref.shape[0])], tok_ref, rem_ref)


def place_into(dst, expert, slot, choices, src, rest):
    toks = src.shape[1]
    none = jnp.zeros((expert.shape[0], toks), F32)

    def matrix(wanted):
        out = none
        for code, prob in choices:
            out = jnp.where(code == wanted, 1.0 if prob is None else prob, out)
        return out.astype(BF)

    main = matrix(jnp.where(slot < CAP, expert * MROWS + slot, -2).astype(code_type(choices)))
    for j in range(3):
        cols = slice(j * CHUNK, (j + 1) * CHUNK)
        extra = matrix(jnp.where(slot >= CAP, expert * MROWS + 3 * (slot - CAP) + j, -2).astype(code_type(choices)))
        dst[:, cols] = (dot_nt(main, src[cols, :]) + dot_nt(extra, rest[...])).astype(BF)
    dst[:, 3 * CHUNK :] = dot_nt(main, src[3 * CHUNK : MAIN, :]).astype(BF)


def code_type(choices):
    return choices[0][0].dtype


def pack(code, tokens_t, experts):
    return pl.pallas_call(
        pack_kernel,
        out_shape=jax.ShapeDtypeStruct((experts * MROWS, MAIN), BF),
        scratch_shapes=[pltpu.VMEM((CHUNK, tokens_t.shape[1]), BF)],
        compiler_params=pltpu.CompilerParams(vmem_limit_bytes=40 * 2**20),
    )(code, tokens_t)


STEPS = (1, 3, 2)
LINE = ((1, 0), (3, 0), (2, 0), (1, 1), (3, 1), (2, 1), (0, 1))
MESH = pl.DeviceIdType.MESH
HALF = MAIN // 2
PARTS = 2
BLOCKS = 8 // PARTS


def exchange_kernel(table_ref, rows_ref, cot_ref, rows_out, wt_out, *scratch):
    (relay_a, held_a, relay_b, cots, tables, sent, rest, block_buf) = scratch[:8]
    (tab_s, tab_r, cot_s, cot_r, a1_s, a1_r, a2_s, a2_r, a3_s, a3_r, b1_s, b1_r, b2_s, b2_r, own) = scratch[8:]
    e, d = lax.axis_index("expert"), lax.axis_index("dp")
    z, y, x, c = e // 16, (e // 4) % 4, d * 2 + (e // 2) % 2, e % 2
    xc, sub = x * 2 + c, (x % 2) * 2 + c

    def device(dz, dy, dx=0, dc=0):
        ox = (x + dx) % 4
        return ((((z + dz) % 4) * 4 + (y + dy) % 4) * 2 + ox % 2) * 2 + (c + dc) % 2, ox // 2

    barrier = pltpu.get_barrier_semaphore()
    for step in STEPS:
        pl.semaphore_signal(barrier, inc=1, device_id=device(step, 0), device_id_type=MESH)
        pl.semaphore_signal(barrier, inc=1, device_id=device(0, step), device_id_type=MESH)
    for off in LINE:
        pl.semaphore_signal(barrier, inc=1, device_id=device(0, 0, *off), device_id_type=MESH)
    pl.semaphore_wait(barrier, 2 * len(STEPS) + len(LINE))

    started = []

    def send(src, dst, ssem, rsem, target):
        copy = pltpu.make_async_remote_copy(
            src_ref=src, dst_ref=dst, send_sem=ssem, recv_sem=rsem, device_id=target, device_id_type=MESH
        )
        copy.start()
        started.append(copy)
        return copy

    local = []

    def keep(src, dst, sem):
        copy = pltpu.make_async_copy(src, dst, sem)
        copy.start()
        local.append(copy)
        return copy

    mine = (z, y)
    halves = (pl.ds(0, HALF), pl.ds(HALF, HALF))

    def at(h, first, second):
        return (first, second) if h == 0 else (second, first)

    def first_step(h, step):
        return device(step, 0) if h == 0 else device(0, step)

    def second_step(h, step):
        return device(0, step) if h == 0 else device(step, 0)

    def pick(ref, h, first, second, *more):
        one, two = at(h, first, second)
        return ref.at[(one, two, *more)]

    every = slice(None)
    keep(cot_ref, cots.at[xc], own.at[0])
    keep(table_ref, tables.at[xc], own.at[1])
    a1 = [[None] * 3, [None] * 3]
    a2 = [[[None] * 3 for _ in range(4)] for _ in range(2)]
    for h in range(2):
        keep(rows_ref.at[z, y, :, :, halves[h]], relay_a.at[h, mine[h], mine[1 - h]], own.at[2 + h])
    for i, off in enumerate(LINE):
        tab = send(table_ref, tables.at[xc], tab_s.at[i], tab_r.at[i], device(0, 0, *off))
    tab_copies = started[-len(LINE) :]
    tail = cot_ref.shape[0] // 2
    parts = (pl.ds(0, tail), pl.ds(tail, tail))

    def send_cot(src, dst, k, target):
        return send(src, dst, cot_s.at[k], cot_r.at[k], target)

    near = [send_cot(cot_ref, cots.at[xc], i, device(0, 0, step)) for i, step in enumerate((1, 3))]
    for i, step in enumerate(STEPS):
        for h in range(2):
            to = (mine[h] + step) % 4
            a1[h][i] = send(
                pick(rows_ref, h, to, every, every, every, halves[h]),
                relay_a.at[h, mine[h]],
                a1_s.at[h, i],
                a1_r.at[h, i],
                first_step(h, step),
            )
    other_core = [send_cot(cot_ref, cots.at[xc], 4, device(0, 0, 0, 1))]

    def forward_rows(h, i, source):
        for j, step in enumerate(STEPS):
            to = (mine[1 - h] + step) % 4
            if source is None:
                src = pick(rows_ref, h, mine[h], to, every, every, halves[h])
                place = mine[h]
            else:
                src = relay_a.at[h, source, to]
                place = source
            a2[h][i][j] = send(src, held_a.at[h, mine[1 - h], place], a2_s.at[h, i, j], a2_r.at[h, i, j], second_step(h, step))

    for h in range(2):
        forward_rows(h, 3, None)
    def forward_a1(i):
        for h in range(2):
            a1[h][i].wait_recv()
            forward_rows(h, i, (mine[h] - STEPS[i]) % 4)

    forward_a1(0)
    forward_a1(1)
    far = []
    for i, step in enumerate((1, 3)):
        block = ((x - step) % 4) * 2 + c
        near[i].wait_recv()
        far.append(send_cot(cots.at[block, parts[i]], cots.at[block, parts[i]], 2 + i, device(0, 0, step)))
        other_core.append(send_cot(cots.at[block], cots.at[block], 5 + i, device(0, 0, 0, 1)))
    forward_a1(2)
    block = ((x + 2) % 4) * 2 + c
    for i in range(2):
        far[i].wait_recv()
        other_core.append(send_cot(cots.at[block, parts[i]], cots.at[block, parts[i]], 7 + i, device(0, 0, 0, 1)))

    def spread_rows(h, group, source, place):
        where = pick(rows_out, h, every, place, xc, every, halves[h])
        for k, off in enumerate(LINE):
            ox, oc = (x + off[0]) % 4, (c + off[1]) % 2
            send(
                source.at[:, (ox % 2) * 2 + oc],
                where,
                a3_s.at[h, group, k],
                a3_r.at[h, group, k],
                device(0, 0, *off),
            )
        keep(source.at[:, sub], where, own.at[4 + 4 * h + group])

    for copy in local[:4]:
        copy.wait()
    for h in range(2):
        spread_rows(h, 3, relay_a.at[h, :, mine[1 - h]], mine[1 - h])

    rest[...] = jnp.zeros_like(rest)
    width = cot_ref.shape[0]
    row = iota((16 * MROWS, 1), 0)

    def make_block(b):
        rest[: width - MAIN, :] = cots[b, MAIN:, :]
        choices = [(tables[b, k : k + 1, :], tables[b, 4 + k : 5 + k, :]) for k in range(4)]
        place_into(block_buf, (row // MROWS) * 4 + sub, row % MROWS, choices, cots.at[b], rest)
        sent[:, :, b] = block_buf[...].reshape(4, 4, MROWS, MAIN)

    for copy in tab_copies + other_core:
        copy.wait_recv()
    b1 = [[[None] * 3, [None] * 3] for _ in range(PARTS)]
    b2 = [[[[None] * 3 for _ in range(4)] for _ in range(2)] for _ in range(PARTS)]

    def forward_wts(p, h, i, source):
        blocks = pl.ds(p * BLOCKS, BLOCKS)
        for j, step in enumerate(STEPS + (0,)):
            to = (mine[1 - h] + step) % 4
            if source is None:
                src = pick(sent, h, mine[h], to, blocks, every, halves[h])
                place = mine[h]
            else:
                src = relay_b.at[h, source, to, blocks]
                place = source
            dst = pick(wt_out, h, place, mine[1 - h], blocks, every, halves[h])
            if step:
                b2[p][h][i][j] = send(src, dst, b2_s.at[p, h, i, j], b2_r.at[p, h, i, j], second_step(h, step))
            else:
                keep(src, dst, own.at[12 + (p * 2 + h) * 4 + i])

    for p in range(PARTS):
        blocks = pl.ds(p * BLOCKS, BLOCKS)

        @pl.loop(p * BLOCKS, (p + 1) * BLOCKS)
        def _(b):
            make_block(b)

        for i, step in enumerate(STEPS):
            for h in range(2):
                to = (mine[h] + step) % 4
                b1[p][h][i] = send(
                    pick(sent, h, to, every, blocks, every, halves[h]),
                    relay_b.at[h, mine[h], :, blocks],
                    b1_s.at[p, h, i],
                    b1_r.at[p, h, i],
                    first_step(h, step),
                )
        for h in range(2):
            forward_wts(p, h, 3, None)

    for j, step in enumerate(STEPS):
        for h in range(2):
            for i in range(4):
                a2[h][i][j].wait_recv()
            place = (mine[1 - h] - step) % 4
            spread_rows(h, j, held_a.at[h, place], place)

    for p in range(PARTS):
        for i, step in enumerate(STEPS):
            for h in range(2):
                b1[p][h][i].wait_recv()
                forward_wts(p, h, i, (mine[h] - step) % 4)

    early = {id(copy) for copy in tab_copies + near + far + other_core}
    for group in a1 + [v for half in a2 for v in half] + [v for part in b1 for v in part]:
        early |= {id(copy) for copy in group}
    for copy in local[4:]:
        copy.wait()
    for copy in started:
        if id(copy) not in early:
            copy.wait_recv()
    for copy in started:
        copy.wait_send()


def exchange(table, rows_msg, cot_t):
    out = jax.ShapeDtypeStruct((4, 4, 8, MROWS, MAIN), BF)
    anywhere = pl.BlockSpec(memory_space=pl.ANY)
    shapes = [(7,), (9,), (2, 3), (2, 4, 3), (2, 4, 7), (PARTS, 2, 3), (PARTS, 2, 4, 3)]
    sems = [pltpu.SemaphoreType.DMA(shape) for shape in shapes for _ in range(2)]
    return pl.pallas_call(
        exchange_kernel,
        in_specs=[anywhere] * 3,
        out_specs=[anywhere] * 2,
        out_shape=[out, out],
        scratch_shapes=[
            pltpu.VMEM((2, 4, 4, 4, MROWS, HALF), BF),
            pltpu.VMEM((2, 4, 4, 4, MROWS, HALF), BF),
            pltpu.VMEM((2, 4, 4, 8, MROWS, HALF), BF),
            pltpu.VMEM((8, *cot_t.shape), BF),
            pltpu.VMEM((8, *table.shape), F32),
            pltpu.VMEM((4, 4, 8, MROWS, MAIN), BF),
            pltpu.VMEM((CHUNK, cot_t.shape[1]), BF),
            pltpu.VMEM((16 * MROWS, MAIN), BF),
            *sems,
            pltpu.SemaphoreType.DMA((12 + 8 * PARTS,)),
        ],
        compiler_params=pltpu.CompilerParams(collective_id=0, has_side_effects=True, vmem_limit_bytes=48 * 2**20),
    )(table, rows_msg.reshape(4, 4, 4, MROWS, MAIN), cot_t)


def picks(out_rows, in_rows, wide, reorder=False):
    if wide:
        q, o = iota((out_rows, in_rows), 0), iota((out_rows, in_rows), 1)
    else:
        o, q = iota((out_rows, in_rows), 0), iota((out_rows, in_rows), 1)
    message = o // CAP
    slot = o - CAP * message
    if reorder:
        at = message % 8
        base = q - MROWS * (message - at + (at % 4) * 2 + at // 4)
    else:
        base = q - MROWS * message
    high = jnp.where(slot >= 3, 1, 0)
    main = jnp.where(base == slot, 1.0, 0.0).astype(BF)
    last = base == CAP + high
    rem = [jnp.where(last & (slot - 3 * high == j), 1.0, 0.0).astype(BF) for j in range(3)]
    return main, rem, jnp.where(last, 1.0, 0.0).astype(BF)


TILE = 192
WIDE = TILE // CAP * MROWS


def expert_kernel(rows_msg, wt_msg, gate_hbm, up_hbm, down_hbm, *refs):
    outs, bufs, sems = refs[:6], refs[6:-2], refs[-2:]
    msg_rows, msg_wt, gate_w, up_w, down_w, rows, weighted, hidden, gate_grad, up_grad, glu, slope, full = bufs
    rows_out, weighted_out, hidden_out, gate_grad_out, up_grad_out, packed_out = outs
    arrive, leave = sems
    total, width = rows.shape
    tiles = total // TILE
    rest = width - MAIN

    def tile_of(i, size):
        return pl.ds(pl.multiple_of(i * size, size), size)

    def fetch(i, src, dst):
        copy = pltpu.make_async_copy(src, dst, arrive.at[i])
        copy.start()
        return copy

    def put(i, src, dst):
        copy = pltpu.make_async_copy(src, dst, leave.at[i])
        copy.start()
        return copy

    got_rows = fetch(0, rows_msg, msg_rows)
    got_gate = fetch(1, gate_hbm, gate_w)
    got_up = fetch(2, up_hbm, up_w)
    got_wt = fetch(3, wt_msg, msg_wt)
    got_down = fetch(4, down_hbm, down_w)
    main, rem, _ = picks(TILE, WIDE, False)

    def unpack(src, dst):
        @pl.loop(0, tiles)
        def _(i):
            wide, tile = tile_of(i, WIDE), tile_of(i, TILE)
            dst[tile, :MAIN] = dot(main, src[wide, :MAIN]).astype(BF)
            part = dot(rem[0], src[wide, :rest])
            for j in (1, 2):
                part = part + dot(rem[j], src[wide, j * CHUNK : j * CHUNK + rest])
            dst[tile, MAIN:] = part.astype(BF)

    got_rows.wait()
    unpack(msg_rows, rows)
    puts = [put(0, rows, rows_out)]
    got_gate.wait()
    glu[...] = dot_nt(rows[...], gate_w[...])
    got_up.wait()
    slope[...] = dot_nt(rows[...], up_w[...])

    @pl.loop(0, tiles)
    def _(i):
        tile = tile_of(i, TILE)
        gate, up = glu[tile, :], slope[tile, :] + 1.0
        sig = jax.nn.sigmoid(ALPHA * gate)
        prod = gate * sig
        hidden[tile, :] = (up * prod).astype(BF)
        glu[tile, :] = prod
        slope[tile, :] = up * (sig + ALPHA * prod * (1.0 - sig))

    puts.append(put(1, hidden, hidden_out))
    got_wt.wait()
    unpack(msg_wt, weighted)
    puts.append(put(2, weighted, weighted_out))
    got_down.wait()
    main_t, rem_t, last_t = picks(WIDE, TILE, True, True)
    spare = MAIN - 3 * CHUNK
    lane = iota((TILE, spare), 1)
    spot = 2 * ((iota((TILE, spare), 0) % CAP) % 3)
    hgrad = dot_nt(weighted[...], down_w[...])
    share = jnp.sum(hgrad * hidden[...].astype(F32), axis=1, keepdims=True)
    up_grad[...] = (hgrad * glu[...]).astype(BF)
    gate_grad[...] = (hgrad * slope[...]).astype(BF)
    puts.append(put(3, gate_grad, gate_grad_out))
    puts.append(put(4, up_grad, up_grad_out))
    full[:, width:] = jnp.zeros((total, full.shape[1] - width), BF)
    for start in range(0, width, 768):
        cols = slice(start, min(width, start + 768))
        full[:, cols] = (dot(gate_grad[...], gate_w[:, cols]) + dot(up_grad[...], up_w[:, cols])).astype(BF)
    for i in range(tiles):
        tile, wide = slice(i * TILE, (i + 1) * TILE), slice(i * WIDE, (i + 1) * WIDE)
        tail = full[tile, MAIN : MAIN + CHUNK]
        for j in range(3):
            cols = slice(j * CHUNK, (j + 1) * CHUNK)
            msg_wt[wide, cols] = (dot(main_t, full[tile, cols]) + dot(rem_t[j], tail)).astype(BF)
        part = share[tile, :]
        head = part.astype(BF).astype(F32)
        pair = jnp.where(lane == spot, head, jnp.where(lane == spot + 1, part - head, 0.0)).astype(BF)
        cols = slice(3 * CHUNK, MAIN)
        msg_wt[wide, cols] = (dot(main_t, full[tile, cols]) + dot(last_t, pair)).astype(BF)
        puts.append(put(5 + i, msg_wt.at[wide], packed_out.at[wide]))
    for copy in puts:
        copy.wait()


def expert(rows_msg, wt_msg, gate_w, up_w, down_w):
    units, width = gate_w.shape
    rows = rows_msg.shape[0] // MROWS * CAP
    anywhere = pl.BlockSpec(memory_space=pl.ANY)
    wide, thin = (rows, width), (rows, units)
    return pl.pallas_call(
        expert_kernel,
        in_specs=[anywhere] * 5,
        out_specs=[anywhere] * 6,
        out_shape=[jax.ShapeDtypeStruct(shape, BF) for shape in (wide, wide, thin, thin, thin, rows_msg.shape)],
        scratch_shapes=[
            *[pltpu.VMEM(rows_msg.shape, BF)] * 2,
            *[pltpu.VMEM((units, width), BF)] * 3,
            *[pltpu.VMEM(wide, BF)] * 2,
            *[pltpu.VMEM(thin, BF)] * 3,
            *[pltpu.VMEM(thin, F32)] * 2,
            pltpu.VMEM((rows, MAIN + CHUNK), BF),
            pltpu.SemaphoreType.DMA((5,)),
            pltpu.SemaphoreType.DMA((5 + rows // TILE,)),
        ],
        compiler_params=pltpu.CompilerParams(vmem_limit_bytes=62 * 2**20),
        cost_estimate=pl.CostEstimate(flops=10 * rows * width * units, bytes_accessed=40 * 2**20, transcendentals=0),
    )(rows_msg, wt_msg, gate_w, up_w, down_w)


def combine_kernel(copies, expert_ref, slot_ref, prob_ref, back_ref, in_ref, prob_out_ref):
    toks, rest = in_ref.shape[0], in_ref.shape[1] - MAIN
    total = back_ref.shape[0]
    col = iota((toks, total), 1)
    message = col // MROWS
    place = col - message * MROWS
    holder = message // copies
    zero = jnp.zeros((toks, total), F32)
    main, rem = zero, [zero] * 3
    sums = []
    lane = iota((toks, 128), 1)
    shares = back_ref[:, 3 * CHUNK : 3 * CHUNK + 128]
    for k in range(expert_ref.shape[1]):
        expert, slot = expert_ref[:, k : k + 1], slot_ref[:, k : k + 1]
        kept = slot >= 0
        mine = holder == jnp.where(kept, expert, -1)
        high = jnp.where(slot >= 3, 1, 0)
        which = slot - 3 * high
        main = jnp.where(mine & (place == slot), 1.0, main)
        tail = mine & (place == CAP + high)
        for j in range(3):
            rem[j] = jnp.where(tail & (which == j), 1.0, rem[j])
        got = dot(jnp.where(tail, 1.0, 0.0).astype(BF), shares)
        got = jnp.where((lane == 2 * which) | (lane == 2 * which + 1), got, 0.0)
        sums.append(jnp.sum(got, axis=1, keepdims=True))
    in_ref[:, :MAIN] = dot(main.astype(BF), back_ref[...]).astype(BF)
    part = dot(rem[0].astype(BF), back_ref[:, :rest])
    for j in (1, 2):
        part = part + dot(rem[j].astype(BF), back_ref[:, j * CHUNK : j * CHUNK + rest])
    in_ref[:, MAIN:] = part.astype(BF)
    choice = iota(prob_ref.shape, 1)
    total_share = jnp.zeros(prob_ref.shape, F32)
    for k, value in enumerate(sums):
        total_share = jnp.where(choice == k, value, total_share)
    prob_out_ref[...] = jnp.where(slot_ref[...] >= 0, total_share / prob_ref[...], 0.0)


def combine(expert_ids, slots, probs, back, width, copies):
    return pl.pallas_call(
        functools.partial(combine_kernel, copies),
        out_shape=(
            jax.ShapeDtypeStruct((expert_ids.shape[0], width), BF),
            jax.ShapeDtypeStruct(probs.shape, F32),
        ),
        compiler_params=pltpu.CompilerParams(vmem_limit_bytes=40 * 2**20),
    )(expert_ids, slots, probs, back)


def body(tokens, cotangent, expert_ids, slots, probs, w_gate, w_up, w_down):
    experts = lax.axis_size("expert")
    copies = lax.axis_size("dp")
    devices = experts * copies
    width = tokens.shape[1]
    gate_w, up_w, down_w = w_gate[0].T, w_up[0].T, w_down[0].T
    rounded = probs.astype(BF).astype(F32)
    code = jnp.where(slots >= 0, expert_ids * MROWS + slots, -1).T
    rows_msg = pack(code, tokens.T, experts)
    table = jnp.concatenate([code.astype(F32), rounded.T], axis=0)
    rows_in, wt_in = exchange(table, rows_msg, cotangent.T)
    rows_in = rows_in.reshape(devices * MROWS, MAIN)
    wt_in = wt_in.reshape(devices * MROWS, MAIN)
    rows, weighted, hidden, gate_grad, up_grad, packed = expert(rows_in, wt_in, gate_w, up_w, down_w)
    back = lax.all_to_all(
        packed.reshape(devices, MROWS, MAIN), ("expert", "dp"), split_axis=0, concat_axis=0, tiled=True
    ).reshape(devices * MROWS, MAIN)
    contract_rows = (((0,), (0,)), ((), ()))
    grad_down = lax.dot_general(weighted, hidden, contract_rows, preferred_element_type=F32).astype(BF)
    grad_gate = lax.dot_general(rows, gate_grad, contract_rows, preferred_element_type=F32).astype(BF)
    grad_up = lax.dot_general(rows, up_grad, contract_rows, preferred_element_type=F32).astype(BF)
    input_grad, prob_grad = combine(expert_ids, slots, rounded, back, width, copies)
    return input_grad, prob_grad, grad_gate[None], grad_up[None], grad_down[None]


def solution(mesh):
    token_spec = P(("expert", "dp"), None)
    weight_spec = P("expert", None, "dp")
    return jax.shard_map(
        body,
        mesh=mesh,
        in_specs=(token_spec,) * 5 + (weight_spec,) * 3,
        out_specs=(token_spec,) * 2 + (weight_spec,) * 3,
        check_vma=False,
    )
```

```python
import functools

import jax
import jax.numpy as jnp
from jax import lax
from jax.experimental import pallas as pl
from jax.experimental.pallas import tpu as pltpu
from jax.sharding import PartitionSpec as P

ALPHA = 1.702
BF = jnp.bfloat16
F32 = jnp.float32
CAP = 6
MROWS = 8
MAIN = 2176
CHUNK = 640
ENDS = 64
BODY = slice(MAIN, MAIN + CHUNK)
LAST = slice(3 * CHUNK, MAIN)


def dot(a, b):
    return jnp.dot(a, b, preferred_element_type=F32)


def dot_nt(a, b):
    return lax.dot_general(a, b, (((1,), (1,)), ((), ())), preferred_element_type=F32)


def iota(shape, dim):
    return lax.broadcasted_iota(jnp.int32, shape, dim)


def pack_kernel(code_ref, tok_ref, rows_ref, rem_ref):
    width, toks = tok_ref.shape
    total = rows_ref.shape[0]
    row = iota((total, 1), 0)
    slot = row % MROWS
    message = row // MROWS
    set_ends(rem_ref, tok_ref)
    place_into(rows_ref, message, slot, [(code_ref[k : k + 1, :], None) for k in range(code_ref.shape[0])], tok_ref, rem_ref)


def set_ends(ends, src):
    toks = src.shape[1]
    ends[...] = jnp.zeros_like(ends)
    for j in range(3):
        ends[j * ENDS : (j + 1) * ENDS, j * toks : (j + 1) * toks] = src[MAIN + CHUNK :, :]


def place_into(dst, expert, slot, choices, src, rest):
    toks = src.shape[1]
    none = jnp.zeros((expert.shape[0], toks), F32)

    def matrix(wanted):
        out = none
        for code, prob in choices:
            out = jnp.where(code == wanted, 1.0 if prob is None else prob, out)
        return out.astype(BF)

    main = matrix(jnp.where(slot < CAP, expert * MROWS + slot, -2).astype(code_type(choices)))
    extras = []
    for j in range(3):
        cols = slice(j * CHUNK, (j + 1) * CHUNK)
        wanted = jnp.where(slot >= CAP, expert * MROWS + 3 * (slot - CAP) + j, -2)
        extras.append(matrix(wanted.astype(code_type(choices))))
        dst[:, cols] = (dot_nt(main, src[cols, :]) + dot_nt(extras[j], src[BODY, :])).astype(BF)
    dst[:, LAST] = (dot_nt(main, src[LAST, :]) + dot_nt(jnp.concatenate(extras, axis=1), rest[...])).astype(BF)


def code_type(choices):
    return choices[0][0].dtype


def pack(code, tokens_t, experts):
    return pl.pallas_call(
        pack_kernel,
        out_shape=jax.ShapeDtypeStruct((experts * MROWS, MAIN), BF),
        scratch_shapes=[pltpu.VMEM((MAIN - 3 * CHUNK, 3 * tokens_t.shape[1]), BF)],
        compiler_params=pltpu.CompilerParams(vmem_limit_bytes=40 * 2**20),
    )(code, tokens_t)


STEPS = (1, 3, 2)
LINE = ((1, 0), (3, 0), (2, 0), (1, 1), (3, 1), (2, 1), (0, 1))
MESH = pl.DeviceIdType.MESH
WIDTHS = (1152, MAIN - 1152)
PARTS = 4
EARLY = True


def exchange_kernel(table_ref, rows_ref, cot_ref, rows_out, wt_out, *scratch):
    relay_a, held_a, relay_b = scratch[:2], scratch[2:4], scratch[4:6]
    (cots, tables, sent, rest, block_buf) = scratch[6:11]
    (tab_s, tab_r, cot_s, cot_r, a1_s, a1_r, a2_s, a2_r, a3_s, a3_r, b1_s, b1_r, b2_s, b2_r, own) = scratch[11:]
    e, d = lax.axis_index("expert"), lax.axis_index("dp")
    z, y, x, c = e // 16, (e // 4) % 4, d * 2 + (e // 2) % 2, e % 2
    xc, sub = x * 2 + c, (x % 2) * 2 + c

    def device(dz, dy, dx=0, dc=0):
        ox = (x + dx) % 4
        return ((((z + dz) % 4) * 4 + (y + dy) % 4) * 2 + ox % 2) * 2 + (c + dc) % 2, ox // 2

    barrier = pltpu.get_barrier_semaphore()
    for step in STEPS:
        pl.semaphore_signal(barrier, inc=1, device_id=device(step, 0), device_id_type=MESH)
        pl.semaphore_signal(barrier, inc=1, device_id=device(0, step), device_id_type=MESH)
    for off in LINE:
        pl.semaphore_signal(barrier, inc=1, device_id=device(0, 0, *off), device_id_type=MESH)
    pl.semaphore_wait(barrier, 2 * len(STEPS) + len(LINE))

    started = []

    def send(src, dst, ssem, rsem, target):
        copy = pltpu.make_async_remote_copy(
            src_ref=src, dst_ref=dst, send_sem=ssem, recv_sem=rsem, device_id=target, device_id_type=MESH
        )
        copy.start()
        started.append(copy)
        return copy

    local = []

    def keep(src, dst, sem):
        copy = pltpu.make_async_copy(src, dst, sem)
        copy.start()
        local.append(copy)
        return copy

    mine = (z, y)
    halves = (pl.ds(0, WIDTHS[0]), pl.ds(*WIDTHS))

    def at(h, first, second):
        return (first, second) if h == 0 else (second, first)

    def first_step(h, step):
        return device(step, 0) if h == 0 else device(0, step)

    def second_step(h, step):
        return device(0, step) if h == 0 else device(step, 0)

    def pick(ref, h, first, second, *more):
        one, two = at(h, first, second)
        return ref.at[(one, two, *more)]

    every = slice(None)
    keep(cot_ref, cots.at[xc], own.at[0])
    keep(table_ref, tables.at[xc], own.at[1])
    a1 = [[None] * 3, [None] * 3]
    a2 = [[[None] * 3 for _ in range(4)] for _ in range(2)]
    for h in range(2):
        keep(rows_ref.at[z, y, :, :, halves[h]], relay_a[h].at[mine[h], mine[1 - h]], own.at[2 + h])
    for i, off in enumerate(LINE):
        tab = send(table_ref, tables.at[xc], tab_s.at[i], tab_r.at[i], device(0, 0, *off))
    tab_copies = started[-len(LINE) :]
    tail = cot_ref.shape[0] // 2
    parts = (pl.ds(0, tail), pl.ds(tail, tail))

    def send_cot(src, dst, k, target):
        return send(src, dst, cot_s.at[k], cot_r.at[k], target)

    near = [send_cot(cot_ref, cots.at[xc], i, device(0, 0, step)) for i, step in enumerate((1, 3))]
    for i, step in enumerate(STEPS):
        for h in range(2):
            to = (mine[h] + step) % 4
            a1[h][i] = send(
                pick(rows_ref, h, to, every, every, every, halves[h]),
                relay_a[h].at[mine[h]],
                a1_s.at[h, i],
                a1_r.at[h, i],
                first_step(h, step),
            )
    other_core = [send_cot(cot_ref, cots.at[xc], 4, device(0, 0, 0, 1))]

    def forward_rows(h, i, source):
        for j, step in enumerate(STEPS):
            to = (mine[1 - h] + step) % 4
            if source is None:
                src = pick(rows_ref, h, mine[h], to, every, every, halves[h])
                place = mine[h]
            else:
                src = relay_a[h].at[source, to]
                place = source
            a2[h][i][j] = send(src, held_a[h].at[mine[1 - h], place], a2_s.at[h, i, j], a2_r.at[h, i, j], second_step(h, step))

    for h in range(2):
        forward_rows(h, 3, None)

    def forward_a1(i):
        for h in range(2):
            a1[h][i].wait_recv()
            forward_rows(h, i, (mine[h] - STEPS[i]) % 4)

    def spread_rows(h, group, source, place):
        where = pick(rows_out, h, every, place, xc, every, halves[h])
        for k, off in enumerate(LINE):
            ox, oc = (x + off[0]) % 4, (c + off[1]) % 2
            send(
                source.at[:, (ox % 2) * 2 + oc],
                where,
                a3_s.at[h, group, k],
                a3_r.at[h, group, k],
                device(0, 0, *off),
            )
        keep(source.at[:, sub], where, own.at[4 + 4 * h + group])

    row = iota((16 * MROWS, 1), 0)

    def make_block(b):
        set_ends(rest, cots.at[b])
        choices = [(tables[b, k : k + 1, :], tables[b, 4 + k : 5 + k, :]) for k in range(4)]
        place_into(block_buf, (row // MROWS) * 4 + sub, row % MROWS, choices, cots.at[b], rest)
        sent[:, :, b] = block_buf[...].reshape(4, 4, MROWS, MAIN)

    b1 = [[[None] * 3, [None] * 3] for _ in range(4)]
    b2 = [[[[None] * 3 for _ in range(4)] for _ in range(2)] for _ in range(4)]

    def blocks_of(p):
        return pl.ds(((x - (0, 1, 3, 2)[p]) % 4) * 2, 2)

    def forward_wts(p, h, i, source):
        blocks = blocks_of(p)
        for j, step in enumerate(STEPS + (0,)):
            to = (mine[1 - h] + step) % 4
            if source is None:
                src = pick(sent, h, mine[h], to, blocks, every, halves[h])
                place = mine[h]
            else:
                src = relay_b[h].at[source, to, blocks]
                place = source
            dst = pick(wt_out, h, place, mine[1 - h], blocks, every, halves[h])
            if step:
                b2[p][h][i][j] = send(src, dst, b2_s.at[p, h, i, j], b2_r.at[p, h, i, j], second_step(h, step))
            else:
                keep(src, dst, own.at[12 + (p * 2 + h) * 4 + i])

    def send_part(p):
        start = ((x - (0, 1, 3, 2)[p]) % 4) * 2

        @pl.loop(0, 2)
        def _(b):
            make_block(start + b)

        for i, step in enumerate(STEPS):
            for h in range(2):
                to = (mine[h] + step) % 4
                b1[p][h][i] = send(
                    pick(sent, h, to, every, blocks_of(p), every, halves[h]),
                    relay_b[h].at[mine[h], :, blocks_of(p)],
                    b1_s.at[p, h, i],
                    b1_r.at[p, h, i],
                    first_step(h, step),
                )
        for h in range(2):
            forward_wts(p, h, 3, None)

    def relay_part(p):
        for i, step in enumerate(STEPS):
            for h in range(2):
                b1[p][h][i].wait_recv()
                forward_wts(p, h, i, (mine[h] - step) % 4)

    for copy in local[:4]:
        copy.wait()
    for copy in tab_copies:
        copy.wait_recv()
    other_core[0].wait_recv()
    if EARLY:
        send_part(0)
    forward_a1(0)
    forward_a1(1)
    far = []
    for i, step in enumerate((1, 3)):
        block = ((x - step) % 4) * 2 + c
        near[i].wait_recv()
        far.append(send_cot(cots.at[block, parts[i]], cots.at[block, parts[i]], 2 + i, device(0, 0, step)))
        other_core.append(send_cot(cots.at[block], cots.at[block], 5 + i, device(0, 0, 0, 1)))
    forward_a1(2)
    for h in range(2):
        spread_rows(h, 3, relay_a[h].at[:, mine[1 - h]], mine[1 - h])
    if not EARLY:
        send_part(0)
    for p in (1, 2):
        other_core[p].wait_recv()
        send_part(p)
    block = ((x + 2) % 4) * 2 + c
    for i in range(2):
        far[i].wait_recv()
        other_core.append(send_cot(cots.at[block, parts[i]], cots.at[block, parts[i]], 7 + i, device(0, 0, 0, 1)))
    for copy in other_core[3:]:
        copy.wait_recv()
    send_part(3)
    if EARLY:
        relay_part(0)
    for j, step in enumerate(STEPS):
        for h in range(2):
            for i in range(4):
                a2[h][i][j].wait_recv()
            place = (mine[1 - h] - step) % 4
            spread_rows(h, j, held_a[h].at[place], place)
    for p in range(1 if EARLY else 0, 4):
        relay_part(p)

    early = {id(copy) for copy in tab_copies + near + far + other_core}
    for group in a1 + [v for half in a2 for v in half] + [v for part in b1 for v in part]:
        early |= {id(copy) for copy in group}
    for copy in local[4:]:
        copy.wait()
    for copy in started:
        if id(copy) not in early:
            copy.wait_recv()
    for copy in started:
        copy.wait_send()


def exchange(table, rows_msg, cot_t):
    out = jax.ShapeDtypeStruct((4, 4, 8, MROWS, MAIN), BF)
    anywhere = pl.BlockSpec(memory_space=pl.ANY)
    shapes = [(7,), (9,), (2, 3), (2, 4, 3), (2, 4, 7), (PARTS, 2, 3), (PARTS, 2, 4, 3)]
    sems = [pltpu.SemaphoreType.DMA(shape) for shape in shapes for _ in range(2)]
    return pl.pallas_call(
        exchange_kernel,
        in_specs=[anywhere] * 3,
        out_specs=[anywhere] * 2,
        out_shape=[out, out],
        scratch_shapes=[
            *[pltpu.VMEM((4, 4, at, MROWS, half), BF) for at in (4, 4, 8) for half in WIDTHS],
            pltpu.VMEM((8, *cot_t.shape), BF),
            pltpu.VMEM((8, *table.shape), F32),
            pltpu.VMEM((4, 4, 8, MROWS, MAIN), BF),
            pltpu.VMEM((MAIN - 3 * CHUNK, 3 * cot_t.shape[1]), BF),
            pltpu.VMEM((16 * MROWS, MAIN), BF),
            *sems,
            pltpu.SemaphoreType.DMA((12 + 8 * PARTS,)),
        ],
        compiler_params=pltpu.CompilerParams(collective_id=0, has_side_effects=True, vmem_limit_bytes=62 * 2**20),
    )(table, rows_msg.reshape(4, 4, 4, MROWS, MAIN), cot_t)


def picks(out_rows, in_rows, wide, reorder=False):
    if wide:
        q, o = iota((out_rows, in_rows), 0), iota((out_rows, in_rows), 1)
    else:
        o, q = iota((out_rows, in_rows), 0), iota((out_rows, in_rows), 1)
    message = o // CAP
    slot = o - CAP * message
    if reorder:
        at = message % 8
        base = q - MROWS * (message - at + (at % 4) * 2 + at // 4)
    else:
        base = q - MROWS * message
    high = jnp.where(slot >= 3, 1, 0)
    main = jnp.where(base == slot, 1.0, 0.0).astype(BF)
    last = base == CAP + high
    rem = [jnp.where(last & (slot - 3 * high == j), 1.0, 0.0).astype(BF) for j in range(3)]
    return main, rem, jnp.where(last, 1.0, 0.0).astype(BF)


TILE = 192
WIDE = TILE // CAP * MROWS


def expert_kernel(rows_msg, wt_msg, gate_hbm, up_hbm, down_hbm, *refs):
    outs, bufs, sems = refs[:6], refs[6:-2], refs[-2:]
    msg_rows, msg_wt, gate_w, up_w, down_w, rows, weighted, hidden, gate_grad, up_grad, glu, slope, full = bufs
    rows_out, weighted_out, hidden_out, gate_grad_out, up_grad_out, packed_out = outs
    arrive, leave = sems
    total, width = rows.shape
    tiles = total // TILE

    def tile_of(i, size):
        return pl.ds(pl.multiple_of(i * size, size), size)

    def fetch(i, src, dst):
        copy = pltpu.make_async_copy(src, dst, arrive.at[i])
        copy.start()
        return copy

    def put(i, src, dst):
        copy = pltpu.make_async_copy(src, dst, leave.at[i])
        copy.start()
        return copy

    got_rows = fetch(0, rows_msg, msg_rows)
    got_gate = fetch(1, gate_hbm, gate_w)
    got_up = fetch(2, up_hbm, up_w)
    got_wt = fetch(3, wt_msg, msg_wt)
    got_down = fetch(4, down_hbm, down_w)
    main, rem, _ = picks(TILE, WIDE, False)

    def unpack(src, dst):
        @pl.loop(0, tiles)
        def _(i):
            wide, tile = tile_of(i, WIDE), tile_of(i, TILE)
            dst[tile, :MAIN] = dot(main, src[wide, :MAIN]).astype(BF)
            part = dot(rem[0], src[wide, :CHUNK])
            for j in (1, 2):
                part = part + dot(rem[j], src[wide, j * CHUNK : (j + 1) * CHUNK])
            dst[tile, BODY] = part.astype(BF)
            one, two = src[wide, 3 * CHUNK : 3 * CHUNK + 128], src[wide, 3 * CHUNK + 128 :]
            ends = dot(rem[0], one) + pltpu.roll(dot(rem[1], one), ENDS, 1) + dot(rem[2], two)
            dst[tile, MAIN + CHUNK :] = ends[:, :ENDS].astype(BF)

    got_rows.wait()
    unpack(msg_rows, rows)
    puts = [put(0, rows, rows_out)]
    got_gate.wait()
    glu[...] = dot_nt(rows[...], gate_w[...])
    got_up.wait()
    slope[...] = dot_nt(rows[...], up_w[...])

    @pl.loop(0, tiles)
    def _(i):
        tile = tile_of(i, TILE)
        gate, up = glu[tile, :], slope[tile, :] + 1.0
        sig = jax.nn.sigmoid(ALPHA * gate)
        prod = gate * sig
        hidden[tile, :] = (up * prod).astype(BF)
        glu[tile, :] = prod
        slope[tile, :] = up * (sig + ALPHA * prod * (1.0 - sig))

    puts.append(put(1, hidden, hidden_out))
    got_wt.wait()
    unpack(msg_wt, weighted)
    puts.append(put(2, weighted, weighted_out))
    got_down.wait()
    main_t, rem_t, last_t = picks(WIDE, TILE, True, True)
    lane = iota((TILE, 128), 1)
    slot = iota((TILE, 128), 0) % CAP
    which = slot % 3
    spot = ENDS + 2 * which
    hgrad = dot_nt(weighted[...], down_w[...])
    share = jnp.sum(hgrad * hidden[...].astype(F32), axis=1, keepdims=True)
    up_grad[...] = (hgrad * glu[...]).astype(BF)
    gate_grad[...] = (hgrad * slope[...]).astype(BF)
    puts.append(put(3, gate_grad, gate_grad_out))
    puts.append(put(4, up_grad, up_grad_out))
    full[:, width:] = jnp.zeros((total, full.shape[1] - width), BF)
    for start in range(0, width, 768):
        cols = slice(start, min(width, start + 768))
        full[:, cols] = (dot(gate_grad[...], gate_w[:, cols]) + dot(up_grad[...], up_w[:, cols])).astype(BF)
    for i in range(tiles):
        tile, wide = slice(i * TILE, (i + 1) * TILE), slice(i * WIDE, (i + 1) * WIDE)
        for j in range(3):
            cols = slice(j * CHUNK, (j + 1) * CHUNK)
            msg_wt[wide, cols] = (dot(main_t, full[tile, cols]) + dot(rem_t[j], full[tile, BODY])).astype(BF)
        part = share[tile, :]
        head = part.astype(BF).astype(F32)
        pair = jnp.where(lane == spot, head, jnp.where(lane == spot + 1, part - head, 0.0))
        ends = full[tile, MAIN + CHUNK :].astype(F32)
        one = jnp.where(which == 0, ends, jnp.where(which == 1, pltpu.roll(ends, ENDS, 1), 0.0))
        two = jnp.where(which == 2, ends, 0.0) + pair
        for k, value in enumerate((one, two)):
            cols = slice(3 * CHUNK + 128 * k, 3 * CHUNK + 128 * (k + 1))
            msg_wt[wide, cols] = (dot(main_t, full[tile, cols]) + dot(last_t, value.astype(BF))).astype(BF)
        puts.append(put(5 + i, msg_wt.at[wide], packed_out.at[wide]))
    for copy in puts:
        copy.wait()


def expert(rows_msg, wt_msg, gate_w, up_w, down_w):
    units, width = gate_w.shape
    rows = rows_msg.shape[0] // MROWS * CAP
    anywhere = pl.BlockSpec(memory_space=pl.ANY)
    wide, thin = (rows, width), (rows, units)
    return pl.pallas_call(
        expert_kernel,
        in_specs=[anywhere] * 5,
        out_specs=[anywhere] * 6,
        out_shape=[jax.ShapeDtypeStruct(shape, BF) for shape in (wide, wide, thin, thin, thin, rows_msg.shape)],
        scratch_shapes=[
            *[pltpu.VMEM(rows_msg.shape, BF)] * 2,
            *[pltpu.VMEM((units, width), BF)] * 3,
            *[pltpu.VMEM(wide, BF)] * 2,
            *[pltpu.VMEM(thin, BF)] * 3,
            *[pltpu.VMEM(thin, F32)] * 2,
            pltpu.VMEM((rows, MAIN + CHUNK + 128), BF),
            pltpu.SemaphoreType.DMA((5,)),
            pltpu.SemaphoreType.DMA((5 + rows // TILE,)),
        ],
        compiler_params=pltpu.CompilerParams(vmem_limit_bytes=62 * 2**20),
        cost_estimate=pl.CostEstimate(flops=10 * rows * width * units, bytes_accessed=40 * 2**20, transcendentals=0),
    )(rows_msg, wt_msg, gate_w, up_w, down_w)


def combine_kernel(copies, expert_ref, slot_ref, prob_ref, back_ref, in_ref, prob_out_ref):
    toks = in_ref.shape[0]
    total = back_ref.shape[0]
    col = iota((toks, total), 1)
    message = col // MROWS
    place = col - message * MROWS
    holder = message // copies
    zero = jnp.zeros((toks, total), F32)
    main, rem = zero, [zero] * 3
    sums = []
    lane = iota((toks, 128), 1)
    first, shares = back_ref[:, 3 * CHUNK : 3 * CHUNK + 128], back_ref[:, 3 * CHUNK + 128 :]
    for k in range(expert_ref.shape[1]):
        expert, slot = expert_ref[:, k : k + 1], slot_ref[:, k : k + 1]
        kept = slot >= 0
        mine = holder == jnp.where(kept, expert, -1)
        high = jnp.where(slot >= 3, 1, 0)
        which = slot - 3 * high
        main = jnp.where(mine & (place == slot), 1.0, main)
        tail = mine & (place == CAP + high)
        for j in range(3):
            rem[j] = jnp.where(tail & (which == j), 1.0, rem[j])
        got = dot(jnp.where(tail, 1.0, 0.0).astype(BF), shares)
        spot = ENDS + 2 * which
        got = jnp.where((lane == spot) | (lane == spot + 1), got, 0.0)
        sums.append(jnp.sum(got, axis=1, keepdims=True))
    in_ref[:, :MAIN] = dot(main.astype(BF), back_ref[...]).astype(BF)
    rem = [value.astype(BF) for value in rem]
    part = dot(rem[0], back_ref[:, :CHUNK])
    for j in (1, 2):
        part = part + dot(rem[j], back_ref[:, j * CHUNK : (j + 1) * CHUNK])
    in_ref[:, BODY] = part.astype(BF)
    ends = dot(rem[0], first) + pltpu.roll(dot(rem[1], first), ENDS, 1) + dot(rem[2], shares)
    in_ref[:, MAIN + CHUNK :] = ends[:, :ENDS].astype(BF)
    choice = iota(prob_ref.shape, 1)
    total_share = jnp.zeros(prob_ref.shape, F32)
    for k, value in enumerate(sums):
        total_share = jnp.where(choice == k, value, total_share)
    prob_out_ref[...] = jnp.where(slot_ref[...] >= 0, total_share / prob_ref[...], 0.0)


def combine(expert_ids, slots, probs, back, width, copies):
    return pl.pallas_call(
        functools.partial(combine_kernel, copies),
        out_shape=(
            jax.ShapeDtypeStruct((expert_ids.shape[0], width), BF),
            jax.ShapeDtypeStruct(probs.shape, F32),
        ),
        compiler_params=pltpu.CompilerParams(vmem_limit_bytes=40 * 2**20),
    )(expert_ids, slots, probs, back)


def body(tokens, cotangent, expert_ids, slots, probs, w_gate, w_up, w_down):
    experts = lax.axis_size("expert")
    copies = lax.axis_size("dp")
    devices = experts * copies
    width = tokens.shape[1]
    gate_w, up_w, down_w = w_gate[0].T, w_up[0].T, w_down[0].T
    rounded = probs.astype(BF).astype(F32)
    code = jnp.where(slots >= 0, expert_ids * MROWS + slots, -1).T
    rows_msg = pack(code, tokens.T, experts)
    table = jnp.concatenate([code.astype(F32), rounded.T], axis=0)
    rows_in, wt_in = exchange(table, rows_msg, cotangent.T)
    rows_in = rows_in.reshape(devices * MROWS, MAIN)
    wt_in = wt_in.reshape(devices * MROWS, MAIN)
    rows, weighted, hidden, gate_grad, up_grad, packed = expert(rows_in, wt_in, gate_w, up_w, down_w)
    back = lax.all_to_all(
        packed.reshape(devices, MROWS, MAIN), ("expert", "dp"), split_axis=0, concat_axis=0, tiled=True
    ).reshape(devices * MROWS, MAIN)
    contract_rows = (((0,), (0,)), ((), ()))
    grad_down = lax.dot_general(weighted, hidden, contract_rows, preferred_element_type=F32).astype(BF)
    grad_gate = lax.dot_general(rows, gate_grad, contract_rows, preferred_element_type=F32).astype(BF)
    grad_up = lax.dot_general(rows, up_grad, contract_rows, preferred_element_type=F32).astype(BF)
    input_grad, prob_grad = combine(expert_ids, slots, rounded, back, width, copies)
    return input_grad, prob_grad, grad_gate[None], grad_up[None], grad_down[None]


def solution(mesh):
    token_spec = P(("expert", "dp"), None)
    weight_spec = P("expert", None, "dp")
    return jax.shard_map(
        body,
        mesh=mesh,
        in_specs=(token_spec,) * 5 + (weight_spec,) * 3,
        out_specs=(token_spec,) * 2 + (weight_spec,) * 3,
        check_vma=False,
    )
```

```python
import functools

import jax
import jax.numpy as jnp
from jax import lax
from jax.experimental import pallas as pl
from jax.experimental.pallas import tpu as pltpu
from jax.sharding import PartitionSpec as P

ALPHA = 1.702
BF = jnp.bfloat16
F32 = jnp.float32
CAP = 6
MROWS = 8
MAIN = 2176
CHUNK = 640
ENDS = 64
BODY = slice(MAIN, MAIN + CHUNK)
LAST = slice(3 * CHUNK, MAIN)


def dot(a, b):
    return jnp.dot(a, b, preferred_element_type=F32)


def dot_nt(a, b):
    return lax.dot_general(a, b, (((1,), (1,)), ((), ())), preferred_element_type=F32)


def iota(shape, dim):
    return lax.broadcasted_iota(jnp.int32, shape, dim)


def pack_kernel(expert_ref, slot_ref, prob_ref, tok_ref, rows_ref, table_ref, rem_ref):
    top = expert_ref.shape[0]
    code = jnp.where(slot_ref[...] >= 0, expert_ref[...] * MROWS + slot_ref[...], -1)
    table_ref[:top, :] = code.astype(F32)
    table_ref[top:, :] = prob_ref[...].astype(BF).astype(F32)
    total = rows_ref.shape[0]
    row = iota((total, 1), 0)
    slot = row % MROWS
    message = row // MROWS
    set_ends(rem_ref, tok_ref)
    place_into(rows_ref, message, slot, [(code[k : k + 1, :], None) for k in range(top)], tok_ref, rem_ref)


def set_ends(ends, src):
    toks = src.shape[1]
    ends[...] = jnp.zeros_like(ends)
    for j in range(3):
        ends[j * ENDS : (j + 1) * ENDS, j * toks : (j + 1) * toks] = src[MAIN + CHUNK :, :]


def place_into(dst, expert, slot, choices, src, rest):
    toks = src.shape[1]
    none = jnp.zeros((expert.shape[0], toks), F32)

    def matrix(wanted):
        out = none
        for code, prob in choices:
            out = jnp.where(code == wanted, 1.0 if prob is None else prob, out)
        return out.astype(BF)

    main = matrix(jnp.where(slot < CAP, expert * MROWS + slot, -2).astype(code_type(choices)))
    extras = []
    for j in range(3):
        cols = slice(j * CHUNK, (j + 1) * CHUNK)
        wanted = jnp.where(slot >= CAP, expert * MROWS + 3 * (slot - CAP) + j, -2)
        extras.append(matrix(wanted.astype(code_type(choices))))
        dst[:, cols] = (dot_nt(main, src[cols, :]) + dot_nt(extras[j], src[BODY, :])).astype(BF)
    dst[:, LAST] = (dot_nt(main, src[LAST, :]) + dot_nt(jnp.concatenate(extras, axis=1), rest[...])).astype(BF)


def code_type(choices):
    return choices[0][0].dtype


def pack(expert_t, slot_t, prob_t, tokens_t, experts):
    return pl.pallas_call(
        pack_kernel,
        out_shape=(
            jax.ShapeDtypeStruct((experts * MROWS, MAIN), BF),
            jax.ShapeDtypeStruct((2 * slot_t.shape[0], slot_t.shape[1]), F32),
        ),
        scratch_shapes=[pltpu.VMEM((MAIN - 3 * CHUNK, 3 * tokens_t.shape[1]), BF)],
        compiler_params=pltpu.CompilerParams(vmem_limit_bytes=67_043_328),
    )(expert_t, slot_t, prob_t, tokens_t)


STEPS = (1, 3, 2)
LINE = ((1, 0), (3, 0), (2, 0), (1, 1), (3, 1), (2, 1), (0, 1))
MESH = pl.DeviceIdType.MESH
WIDTHS = (1152, MAIN - 1152)
PARTS = 4
EARLY = True


def exchange_kernel(table_ref, rows_ref, cot_ref, rows_out, wt_out, *scratch):
    relay_a, held_a, relay_b = scratch[:2], scratch[2:4], scratch[4:6]
    (cots, tables, sent, rest, block_buf) = scratch[6:11]
    (tab_s, tab_r, cot_s, cot_r, a1_s, a1_r, a2_s, a2_r, a3_s, a3_r, b1_s, b1_r, b2_s, b2_r, own) = scratch[11:]
    e, d = lax.axis_index("expert"), lax.axis_index("dp")
    z, y, x, c = e // 16, (e // 4) % 4, d * 2 + (e // 2) % 2, e % 2
    xc, sub = x * 2 + c, (x % 2) * 2 + c

    def device(dz, dy, dx=0, dc=0):
        ox = (x + dx) % 4
        return ((((z + dz) % 4) * 4 + (y + dy) % 4) * 2 + ox % 2) * 2 + (c + dc) % 2, ox // 2

    barrier = pltpu.get_barrier_semaphore()
    for step in STEPS:
        pl.semaphore_signal(barrier, inc=1, device_id=device(step, 0), device_id_type=MESH)
        pl.semaphore_signal(barrier, inc=1, device_id=device(0, step), device_id_type=MESH)
    for off in LINE:
        pl.semaphore_signal(barrier, inc=1, device_id=device(0, 0, *off), device_id_type=MESH)
    pl.semaphore_wait(barrier, 2 * len(STEPS) + len(LINE))

    started = []

    def send(src, dst, ssem, rsem, target):
        copy = pltpu.make_async_remote_copy(
            src_ref=src, dst_ref=dst, send_sem=ssem, recv_sem=rsem, device_id=target, device_id_type=MESH
        )
        copy.start()
        started.append(copy)
        return copy

    local = []

    def keep(src, dst, sem):
        copy = pltpu.make_async_copy(src, dst, sem)
        copy.start()
        local.append(copy)
        return copy

    mine = (z, y)
    halves = (pl.ds(0, WIDTHS[0]), pl.ds(*WIDTHS))

    def at(h, first, second):
        return (first, second) if h == 0 else (second, first)

    def first_step(h, step):
        return device(step, 0) if h == 0 else device(0, step)

    def second_step(h, step):
        return device(0, step) if h == 0 else device(step, 0)

    def pick(ref, h, first, second, *more):
        one, two = at(h, first, second)
        return ref.at[(one, two, *more)]

    every = slice(None)
    keep(cot_ref, cots.at[xc], own.at[0])
    keep(table_ref, tables.at[xc], own.at[1])
    a1 = [[None] * 3, [None] * 3]
    a2 = [[[None] * 3 for _ in range(4)] for _ in range(2)]
    for h in range(2):
        keep(rows_ref.at[z, y, :, :, halves[h]], relay_a[h].at[mine[h], mine[1 - h]], own.at[2 + h])
    for i, off in enumerate(LINE):
        tab = send(table_ref, tables.at[xc], tab_s.at[i], tab_r.at[i], device(0, 0, *off))
    tab_copies = started[-len(LINE) :]
    tail = cot_ref.shape[0] // 2
    parts = (pl.ds(0, tail), pl.ds(tail, tail))

    def send_cot(src, dst, k, target):
        return send(src, dst, cot_s.at[k], cot_r.at[k], target)

    near = [send_cot(cot_ref, cots.at[xc], i, device(0, 0, step)) for i, step in enumerate((1, 3))]
    for i, step in enumerate(STEPS):
        for h in range(2):
            to = (mine[h] + step) % 4
            a1[h][i] = send(
                pick(rows_ref, h, to, every, every, every, halves[h]),
                relay_a[h].at[mine[h]],
                a1_s.at[h, i],
                a1_r.at[h, i],
                first_step(h, step),
            )
    other_core = [send_cot(cot_ref, cots.at[xc], 4, device(0, 0, 0, 1))]

    def forward_rows(h, i, source):
        for j, step in enumerate(STEPS):
            to = (mine[1 - h] + step) % 4
            if source is None:
                src = pick(rows_ref, h, mine[h], to, every, every, halves[h])
                place = mine[h]
            else:
                src = relay_a[h].at[source, to]
                place = source
            a2[h][i][j] = send(src, held_a[h].at[mine[1 - h], place], a2_s.at[h, i, j], a2_r.at[h, i, j], second_step(h, step))

    for h in range(2):
        forward_rows(h, 3, None)

    def forward_a1(i):
        for h in range(2):
            a1[h][i].wait_recv()
            forward_rows(h, i, (mine[h] - STEPS[i]) % 4)

    def spread_rows(h, group, source, place):
        where = pick(rows_out, h, every, place, xc, every, halves[h])
        for k, off in enumerate(LINE):
            ox, oc = (x + off[0]) % 4, (c + off[1]) % 2
            send(
                source.at[:, (ox % 2) * 2 + oc],
                where,
                a3_s.at[h, group, k],
                a3_r.at[h, group, k],
                device(0, 0, *off),
            )
        keep(source.at[:, sub], where, own.at[4 + 4 * h + group])

    row = iota((16 * MROWS, 1), 0)

    def make_block(b):
        set_ends(rest, cots.at[b])
        choices = [(tables[b, k : k + 1, :], tables[b, 4 + k : 5 + k, :]) for k in range(4)]
        place_into(block_buf, (row // MROWS) * 4 + sub, row % MROWS, choices, cots.at[b], rest)
        sent[:, :, b] = block_buf[...].reshape(4, 4, MROWS, MAIN)

    b1 = [[[None] * 3, [None] * 3] for _ in range(4)]
    b2 = [[[[None] * 3 for _ in range(4)] for _ in range(2)] for _ in range(4)]

    def blocks_of(p):
        return pl.ds(((x - (0, 1, 3, 2)[p]) % 4) * 2, 2)

    def forward_wts(p, h, i, source):
        blocks = blocks_of(p)
        for j, step in enumerate(STEPS + (0,)):
            to = (mine[1 - h] + step) % 4
            if source is None:
                src = pick(sent, h, mine[h], to, blocks, every, halves[h])
                place = mine[h]
            else:
                src = relay_b[h].at[source, to, blocks]
                place = source
            dst = pick(wt_out, h, place, mine[1 - h], blocks, every, halves[h])
            if step:
                b2[p][h][i][j] = send(src, dst, b2_s.at[p, h, i, j], b2_r.at[p, h, i, j], second_step(h, step))
            else:
                keep(src, dst, own.at[12 + (p * 2 + h) * 4 + i])

    def send_part(p):
        start = ((x - (0, 1, 3, 2)[p]) % 4) * 2

        @pl.loop(0, 2)
        def _(b):
            make_block(start + b)

        for i, step in enumerate(STEPS):
            for h in range(2):
                to = (mine[h] + step) % 4
                b1[p][h][i] = send(
                    pick(sent, h, to, every, blocks_of(p), every, halves[h]),
                    relay_b[h].at[mine[h], :, blocks_of(p)],
                    b1_s.at[p, h, i],
                    b1_r.at[p, h, i],
                    first_step(h, step),
                )
        for h in range(2):
            forward_wts(p, h, 3, None)

    def relay_part(p):
        for i, step in enumerate(STEPS):
            for h in range(2):
                b1[p][h][i].wait_recv()
                forward_wts(p, h, i, (mine[h] - step) % 4)

    for copy in local[:4]:
        copy.wait()
    for copy in tab_copies:
        copy.wait_recv()
    other_core[0].wait_recv()
    if EARLY:
        send_part(0)
    forward_a1(0)
    forward_a1(1)
    far = []
    for i, step in enumerate((1, 3)):
        block = ((x - step) % 4) * 2 + c
        near[i].wait_recv()
        far.append(send_cot(cots.at[block, parts[i]], cots.at[block, parts[i]], 2 + i, device(0, 0, step)))
        other_core.append(send_cot(cots.at[block], cots.at[block], 5 + i, device(0, 0, 0, 1)))
    forward_a1(2)
    for h in range(2):
        spread_rows(h, 3, relay_a[h].at[:, mine[1 - h]], mine[1 - h])
    if not EARLY:
        send_part(0)
    for p in (1, 2):
        other_core[p].wait_recv()
        send_part(p)
    block = ((x + 2) % 4) * 2 + c
    for i in range(2):
        far[i].wait_recv()
        other_core.append(send_cot(cots.at[block, parts[i]], cots.at[block, parts[i]], 7 + i, device(0, 0, 0, 1)))
    for copy in other_core[3:]:
        copy.wait_recv()
    send_part(3)
    if EARLY:
        relay_part(0)
    for j, step in enumerate(STEPS):
        for h in range(2):
            for i in range(4):
                a2[h][i][j].wait_recv()
            place = (mine[1 - h] - step) % 4
            spread_rows(h, j, held_a[h].at[place], place)
    for p in range(1 if EARLY else 0, 4):
        relay_part(p)

    early = {id(copy) for copy in tab_copies + near + far + other_core}
    for group in a1 + [v for half in a2 for v in half] + [v for part in b1 for v in part]:
        early |= {id(copy) for copy in group}
    for copy in local[4:]:
        copy.wait()
    for copy in started:
        if id(copy) not in early:
            copy.wait_recv()
    for copy in started:
        copy.wait_send()


def exchange(table, rows_msg, cot_t):
    out = jax.ShapeDtypeStruct((4, 4, 8, MROWS, MAIN), BF)
    anywhere = pl.BlockSpec(memory_space=pl.ANY)
    shapes = [(7,), (9,), (2, 3), (2, 4, 3), (2, 4, 7), (PARTS, 2, 3), (PARTS, 2, 4, 3)]
    sems = [pltpu.SemaphoreType.DMA(shape) for shape in shapes for _ in range(2)]
    return pl.pallas_call(
        exchange_kernel,
        in_specs=[anywhere] * 3,
        out_specs=[anywhere] * 2,
        out_shape=[out, out],
        scratch_shapes=[
            *[pltpu.VMEM((4, 4, at, MROWS, half), BF) for at in (4, 4, 8) for half in WIDTHS],
            pltpu.VMEM((8, *cot_t.shape), BF),
            pltpu.VMEM((8, *table.shape), F32),
            pltpu.VMEM((4, 4, 8, MROWS, MAIN), BF),
            pltpu.VMEM((MAIN - 3 * CHUNK, 3 * cot_t.shape[1]), BF),
            pltpu.VMEM((16 * MROWS, MAIN), BF),
            *sems,
            pltpu.SemaphoreType.DMA((12 + 8 * PARTS,)),
        ],
        compiler_params=pltpu.CompilerParams(collective_id=0, has_side_effects=True, vmem_limit_bytes=67_043_328),
    )(table, rows_msg.reshape(4, 4, 4, MROWS, MAIN), cot_t)


def picks(out_rows, in_rows, wide, reorder=False):
    if wide:
        q, o = iota((out_rows, in_rows), 0), iota((out_rows, in_rows), 1)
    else:
        o, q = iota((out_rows, in_rows), 0), iota((out_rows, in_rows), 1)
    message = o // CAP
    slot = o - CAP * message
    if reorder:
        at = message % 8
        base = q - MROWS * (message - at + (at % 4) * 2 + at // 4)
    else:
        base = q - MROWS * message
    high = jnp.where(slot >= 3, 1, 0)
    main = jnp.where(base == slot, 1.0, 0.0).astype(BF)
    last = base == CAP + high
    rem = [jnp.where(last & (slot - 3 * high == j), 1.0, 0.0).astype(BF) for j in range(3)]
    return main, rem, jnp.where(last, 1.0, 0.0).astype(BF)


TILE = 192
WIDE = TILE // CAP * MROWS


def expert_kernel(rows_msg, wt_msg, gate_hbm, up_hbm, down_hbm, *refs):
    outs, bufs, sems = refs[:6], refs[6:-2], refs[-2:]
    msg_rows, msg_wt, gate_w, up_w, down_w, rows, weighted, hidden, gate_grad, up_grad, glu, slope, full, shares = bufs
    rows_out, weighted_out, hidden_out, gate_grad_out, up_grad_out, packed_out = outs
    arrive, leave = sems
    total, width = rows.shape
    tiles = total // TILE

    def tile_of(i, size):
        return pl.ds(pl.multiple_of(i * size, size), size)

    def fetch(i, src, dst):
        copy = pltpu.make_async_copy(src, dst, arrive.at[i])
        copy.start()
        return copy

    def put(i, src, dst):
        copy = pltpu.make_async_copy(src, dst, leave.at[i])
        copy.start()
        return copy

    got_rows = fetch(0, rows_msg, msg_rows)
    got_gate = fetch(1, gate_hbm, gate_w)
    got_up = fetch(2, up_hbm, up_w)
    got_wt = fetch(3, wt_msg, msg_wt)
    got_down = fetch(4, down_hbm, down_w)
    main, rem, _ = picks(TILE, WIDE, False)

    def unpack(src, dst):
        @pl.loop(0, tiles)
        def _(i):
            wide, tile = tile_of(i, WIDE), tile_of(i, TILE)
            dst[tile, :MAIN] = dot(main, src[wide, :MAIN]).astype(BF)
            part = dot(rem[0], src[wide, :CHUNK])
            for j in (1, 2):
                part = part + dot(rem[j], src[wide, j * CHUNK : (j + 1) * CHUNK])
            dst[tile, BODY] = part.astype(BF)
            one, two = src[wide, 3 * CHUNK : 3 * CHUNK + 128], src[wide, 3 * CHUNK + 128 :]
            ends = dot(rem[0], one) + pltpu.roll(dot(rem[1], one), ENDS, 1) + dot(rem[2], two)
            dst[tile, MAIN + CHUNK :] = ends[:, :ENDS].astype(BF)

    got_rows.wait()
    unpack(msg_rows, rows)
    puts = [put(0, rows, rows_out)]
    got_gate.wait()
    glu[...] = dot_nt(rows[...], gate_w[...])
    got_up.wait()
    slope[...] = dot_nt(rows[...], up_w[...])

    @pl.loop(0, tiles)
    def _(i):
        tile = tile_of(i, TILE)
        gate, up = glu[tile, :], slope[tile, :] + 1.0
        sig = jax.nn.sigmoid(ALPHA * gate)
        prod = gate * sig
        hidden[tile, :] = (up * prod).astype(BF)
        glu[tile, :] = prod
        slope[tile, :] = up * (sig + ALPHA * prod * (1.0 - sig))

    puts.append(put(1, hidden, hidden_out))
    got_wt.wait()
    unpack(msg_wt, weighted)
    puts.append(put(2, weighted, weighted_out))
    got_down.wait()
    main_t, rem_t, last_t = picks(WIDE, TILE, True, True)
    lane = iota((TILE, 128), 1)
    slot = iota((TILE, 128), 0) % CAP
    which = slot % 3
    spot = ENDS + 2 * which
    hgrad = dot_nt(weighted[...], down_w[...])
    share = jnp.sum(hgrad * hidden[...].astype(F32), axis=1, keepdims=True)
    up_grad[...] = (hgrad * glu[...]).astype(BF)
    gate_grad[...] = (hgrad * slope[...]).astype(BF)
    puts.append(put(3, gate_grad, gate_grad_out))
    puts.append(put(4, up_grad, up_grad_out))
    full[:, width:] = jnp.zeros((total, full.shape[1] - width), BF)
    for start in range(0, width, 768):
        cols = slice(start, min(width, start + 768))
        full[:, cols] = (dot(gate_grad[...], gate_w[:, cols]) + dot(up_grad[...], up_w[:, cols])).astype(BF)
    shares[...] = jnp.broadcast_to(share, shares.shape)

    @pl.loop(0, tiles)
    def _(i):
        tile, wide = tile_of(i, TILE), tile_of(i, WIDE)
        for j in range(3):
            cols = slice(j * CHUNK, (j + 1) * CHUNK)
            msg_wt[wide, cols] = (dot(main_t, full[tile, cols]) + dot(rem_t[j], full[tile, BODY])).astype(BF)
        part = shares[tile, :]
        head = part.astype(BF).astype(F32)
        pair = jnp.where(lane == spot, head, jnp.where(lane == spot + 1, part - head, 0.0))
        ends = full[tile, MAIN + CHUNK :].astype(F32)
        one = jnp.where(which == 0, ends, jnp.where(which == 1, pltpu.roll(ends, ENDS, 1), 0.0))
        two = jnp.where(which == 2, ends, 0.0) + pair
        for k, value in enumerate((one, two)):
            cols = slice(3 * CHUNK + 128 * k, 3 * CHUNK + 128 * (k + 1))
            msg_wt[wide, cols] = (dot(main_t, full[tile, cols]) + dot(last_t, value.astype(BF))).astype(BF)
        put(5 + i, msg_wt.at[wide], packed_out.at[wide])

    @pl.loop(0, tiles)
    def _(i):
        wide = tile_of(i, WIDE)
        pltpu.make_async_copy(msg_wt.at[wide], packed_out.at[wide], leave.at[5 + i]).wait()

    for copy in puts:
        copy.wait()


def expert(rows_msg, wt_msg, gate_w, up_w, down_w):
    units, width = gate_w.shape
    rows = rows_msg.shape[0] // MROWS * CAP
    anywhere = pl.BlockSpec(memory_space=pl.ANY)
    wide, thin = (rows, width), (rows, units)
    return pl.pallas_call(
        expert_kernel,
        in_specs=[anywhere] * 5,
        out_specs=[anywhere] * 6,
        out_shape=[jax.ShapeDtypeStruct(shape, BF) for shape in (wide, wide, thin, thin, thin, rows_msg.shape)],
        scratch_shapes=[
            *[pltpu.VMEM(rows_msg.shape, BF)] * 2,
            *[pltpu.VMEM((units, width), BF)] * 3,
            *[pltpu.VMEM(wide, BF)] * 2,
            *[pltpu.VMEM(thin, BF)] * 3,
            *[pltpu.VMEM(thin, F32)] * 2,
            pltpu.VMEM((rows, MAIN + CHUNK + 128), BF),
            pltpu.VMEM((rows, 128), F32),
            pltpu.SemaphoreType.DMA((5,)),
            pltpu.SemaphoreType.DMA((5 + rows // TILE,)),
        ],
        compiler_params=pltpu.CompilerParams(vmem_limit_bytes=62 * 2**20),
        cost_estimate=pl.CostEstimate(flops=10 * rows * width * units, bytes_accessed=40 * 2**20, transcendentals=0),
    )(rows_msg, wt_msg, gate_w, up_w, down_w)


def combine_kernel(copies, expert_ref, slot_ref, slot_t_ref, prob_t_ref, back_hbm, in_ref, prob_out_ref, back_ref, sem):
    arrive = pltpu.make_async_copy(back_hbm, back_ref, sem)
    arrive.start()
    toks = in_ref.shape[0]
    total = back_ref.shape[0]
    col = iota((toks, total), 1)
    message = col // MROWS
    place = col - message * MROWS
    holder = message // copies
    zero = jnp.zeros((toks, total), F32)
    main, rem = zero, [zero] * 3
    sums = []
    lane = iota((toks, 128), 1)
    for k in range(expert_ref.shape[1]):
        expert, slot = expert_ref[:, k : k + 1], slot_ref[:, k : k + 1]
        kept = slot >= 0
        mine = holder == jnp.where(kept, expert, -1)
        high = jnp.where(slot >= 3, 1, 0)
        which = slot - 3 * high
        main = jnp.where(mine & (place == slot), 1.0, main)
        tail = mine & (place == CAP + high)
        for j in range(3):
            rem[j] = jnp.where(tail & (which == j), 1.0, rem[j])
        sums.append((jnp.where(tail, 1.0, 0.0).astype(BF), ENDS + 2 * which))
    main = main.astype(BF)
    rem = [value.astype(BF) for value in rem]
    arrive.wait()
    first, shares = back_ref[:, 3 * CHUNK : 3 * CHUNK + 128], back_ref[:, 3 * CHUNK + 128 :]
    in_ref[:, :MAIN] = dot(main, back_ref[...]).astype(BF)
    part = dot(rem[0], back_ref[:, :CHUNK])
    for j in (1, 2):
        part = part + dot(rem[j], back_ref[:, j * CHUNK : (j + 1) * CHUNK])
    in_ref[:, BODY] = part.astype(BF)
    ends = dot(rem[0], first) + pltpu.roll(dot(rem[1], first), ENDS, 1) + dot(rem[2], shares)
    in_ref[:, MAIN + CHUNK :] = ends[:, :ENDS].astype(BF)
    total_share = jnp.zeros((toks, 128), F32)
    for k, (tail, spot) in enumerate(sums):
        got = dot(tail, shares)
        got = jnp.where((lane == spot) | (lane == spot + 1), got, 0.0)
        total_share = jnp.where(lane == k, jnp.sum(got, axis=1, keepdims=True), total_share)
    share_t = total_share.T[: prob_out_ref.shape[0], :]
    rounded = prob_t_ref[...].astype(BF).astype(F32)
    prob_out_ref[...] = jnp.where(slot_t_ref[...] >= 0, share_t / rounded, 0.0)


def combine(expert_ids, slots, probs, back, width, copies):
    return pl.pallas_call(
        functools.partial(combine_kernel, copies),
        out_shape=(
            jax.ShapeDtypeStruct((expert_ids.shape[0], width), BF),
            jax.ShapeDtypeStruct(probs.T.shape, F32),
        ),
        in_specs=[*[pl.BlockSpec(memory_space=pltpu.VMEM)] * 4, pl.BlockSpec(memory_space=pl.ANY)],
        scratch_shapes=[pltpu.VMEM(back.shape, BF), pltpu.SemaphoreType.DMA],
        compiler_params=pltpu.CompilerParams(vmem_limit_bytes=40 * 2**20),
    )(expert_ids, slots, slots.T, probs.T, back)


def body(tokens, cotangent, expert_ids, slots, probs, w_gate, w_up, w_down):
    experts = lax.axis_size("expert")
    copies = lax.axis_size("dp")
    devices = experts * copies
    width = tokens.shape[1]
    gate_w, up_w, down_w = w_gate[0].T, w_up[0].T, w_down[0].T
    rows_msg, table = pack(expert_ids.T, slots.T, probs.T, tokens.T, experts)
    rows_in, wt_in = exchange(table, rows_msg, cotangent.T)
    rows_in = rows_in.reshape(devices * MROWS, MAIN)
    wt_in = wt_in.reshape(devices * MROWS, MAIN)
    rows, weighted, hidden, gate_grad, up_grad, packed = expert(rows_in, wt_in, gate_w, up_w, down_w)
    back = lax.all_to_all(
        packed.reshape(devices, MROWS, MAIN), ("expert", "dp"), split_axis=0, concat_axis=0, tiled=True
    ).reshape(devices * MROWS, MAIN)
    contract_rows = (((0,), (0,)), ((), ()))
    grad_down = lax.dot_general(weighted, hidden, contract_rows, preferred_element_type=F32).astype(BF)
    grad_gate = lax.dot_general(rows, gate_grad, contract_rows, preferred_element_type=F32).astype(BF)
    grad_up = lax.dot_general(rows, up_grad, contract_rows, preferred_element_type=F32).astype(BF)
    input_grad, prob_grad = combine(expert_ids, slots, probs, back, width, copies)
    return input_grad, prob_grad.T, grad_gate[None], grad_up[None], grad_down[None]


def solution(mesh):
    token_spec = P(("expert", "dp"), None)
    weight_spec = P("expert", None, "dp")
    return jax.shard_map(
        body,
        mesh=mesh,
        in_specs=(token_spec,) * 5 + (weight_spec,) * 3,
        out_specs=(token_spec,) * 2 + (weight_spec,) * 3,
        check_vma=False,
    )
```

```python
import functools

import jax
import jax.numpy as jnp
from jax import lax
from jax.experimental import pallas as pl
from jax.experimental.pallas import tpu as pltpu
from jax.sharding import PartitionSpec as P

ALPHA = 1.702
BF = jnp.bfloat16
F32 = jnp.float32
CAP = 6
MROWS = 8
MAIN = 2176
CHUNK = 640
ENDS = 64
BODY = slice(MAIN, MAIN + CHUNK)
LAST = slice(3 * CHUNK, MAIN)


def dot(a, b):
    return jnp.dot(a, b, preferred_element_type=F32)


def dot_nt(a, b):
    return lax.dot_general(a, b, (((1,), (1,)), ((), ())), preferred_element_type=F32)


def iota(shape, dim):
    return lax.broadcasted_iota(jnp.int32, shape, dim)


TILE = 192
WIDE = TILE // CAP * MROWS


def tile_of(i, size):
    return pl.ds(pl.multiple_of(i * size, size), size)


def picks(out_rows, in_rows, wide, reorder=False):
    if wide:
        q, o = iota((out_rows, in_rows), 0), iota((out_rows, in_rows), 1)
    else:
        o, q = iota((out_rows, in_rows), 0), iota((out_rows, in_rows), 1)
    message = o // CAP
    slot = o - CAP * message
    if reorder:
        at = message % 8
        base = q - MROWS * (message - at + (at % 4) * 2 + at // 4)
    else:
        base = q - MROWS * message
    high = jnp.where(slot >= 3, 1, 0)
    main = jnp.where(base == slot, 1.0, 0.0).astype(BF)
    last = base == CAP + high
    rem = [jnp.where(last & (slot - 3 * high == j), 1.0, 0.0).astype(BF) for j in range(3)]
    return main, rem, jnp.where(last, 1.0, 0.0).astype(BF)


def unpack(src, dst, start, stop):
    main, rem, _ = picks(TILE, WIDE, False)

    @pl.loop(0, dst.shape[0] // TILE)
    def _(i):
        wide, tile = tile_of(i, WIDE), tile_of(i, TILE)
        dst[tile, start:stop] = dot(main, src[wide, start:stop]).astype(BF)
        if stop < MAIN:
            return
        part = dot(rem[0], src[wide, :CHUNK])
        for j in (1, 2):
            part = part + dot(rem[j], src[wide, j * CHUNK : (j + 1) * CHUNK])
        dst[tile, BODY] = part.astype(BF)
        one, two = src[wide, 3 * CHUNK : 3 * CHUNK + 128], src[wide, 3 * CHUNK + 128 :]
        ends = dot(rem[0], one) + pltpu.roll(dot(rem[1], one), ENDS, 1) + dot(rem[2], two)
        dst[tile, MAIN + CHUNK :] = ends[:, :ENDS].astype(BF)


def pack_kernel(expert_ref, slot_ref, prob_ref, tok_ref, rows_ref, table_ref, rem_ref):
    top = expert_ref.shape[0]
    code = jnp.where(slot_ref[...] >= 0, expert_ref[...] * MROWS + slot_ref[...], -1)
    table_ref[:top, :] = code.astype(F32)
    table_ref[top:, :] = prob_ref[...].astype(BF).astype(F32)
    total = rows_ref.shape[0]
    row = iota((total, 1), 0)
    slot = row % MROWS
    message = row // MROWS
    set_ends(rem_ref, tok_ref)
    place_into(rows_ref, message, slot, [(code[k : k + 1, :], None) for k in range(top)], tok_ref, rem_ref)


def set_ends(ends, src):
    toks = src.shape[1]
    ends[...] = jnp.zeros_like(ends)
    for j in range(3):
        ends[j * ENDS : (j + 1) * ENDS, j * toks : (j + 1) * toks] = src[MAIN + CHUNK :, :]


def place_into(dst, expert, slot, choices, src, rest):
    toks = src.shape[1]
    none = jnp.zeros((expert.shape[0], toks), F32)

    def matrix(wanted):
        out = none
        for code, prob in choices:
            out = jnp.where(code == wanted, 1.0 if prob is None else prob, out)
        return out.astype(BF)

    main = matrix(jnp.where(slot < CAP, expert * MROWS + slot, -2).astype(code_type(choices)))
    extras = []
    for j in range(3):
        cols = slice(j * CHUNK, (j + 1) * CHUNK)
        wanted = jnp.where(slot >= CAP, expert * MROWS + 3 * (slot - CAP) + j, -2)
        extras.append(matrix(wanted.astype(code_type(choices))))
        dst[:, cols] = (dot_nt(main, src[cols, :]) + dot_nt(extras[j], src[BODY, :])).astype(BF)
    dst[:, LAST] = (dot_nt(main, src[LAST, :]) + dot_nt(jnp.concatenate(extras, axis=1), rest[...])).astype(BF)


def code_type(choices):
    return choices[0][0].dtype


def pack(expert_t, slot_t, prob_t, tokens_t, experts):
    return pl.pallas_call(
        pack_kernel,
        out_shape=(
            jax.ShapeDtypeStruct((experts * MROWS, MAIN), BF),
            jax.ShapeDtypeStruct((2 * slot_t.shape[0], slot_t.shape[1]), F32),
        ),
        scratch_shapes=[pltpu.VMEM((MAIN - 3 * CHUNK, 3 * tokens_t.shape[1]), BF)],
        compiler_params=pltpu.CompilerParams(vmem_limit_bytes=67_043_328),
    )(expert_t, slot_t, prob_t, tokens_t)


STEPS = (1, 3, 2)
LINE = ((1, 0), (3, 0), (2, 0), (1, 1), (3, 1), (2, 1), (0, 1))
MESH = pl.DeviceIdType.MESH
WIDTHS = (1152, MAIN - 1152)
PARTS = 4
EARLY = True


def exchange_kernel(table_ref, rows_ref, cot_ref, gate_hbm, up_hbm, wt_out, full_out, hidden_out, glu_out, slope_out, *scratch):
    relay_a, held_a, relay_b = scratch[:2], scratch[2:4], scratch[4:6]
    (cots, tables, sent, rest, block_buf) = scratch[6:11]
    (rows_out, gate_w, up_w, full_rows, hidden, glu, slope) = scratch[11:18]
    (tab_s, tab_r, cot_s, cot_r, a1_s, a1_r, a2_s, a2_r, a3_s, a3_r, b1_s, b1_r, b2_s, b2_r, own) = scratch[18:]
    e, d = lax.axis_index("expert"), lax.axis_index("dp")
    z, y, x, c = e // 16, (e // 4) % 4, d * 2 + (e // 2) % 2, e % 2
    xc, sub = x * 2 + c, (x % 2) * 2 + c

    def device(dz, dy, dx=0, dc=0):
        ox = (x + dx) % 4
        return ((((z + dz) % 4) * 4 + (y + dy) % 4) * 2 + ox % 2) * 2 + (c + dc) % 2, ox // 2

    barrier = pltpu.get_barrier_semaphore()
    for step in STEPS:
        pl.semaphore_signal(barrier, inc=1, device_id=device(step, 0), device_id_type=MESH)
        pl.semaphore_signal(barrier, inc=1, device_id=device(0, step), device_id_type=MESH)
    for off in LINE:
        pl.semaphore_signal(barrier, inc=1, device_id=device(0, 0, *off), device_id_type=MESH)
    pl.semaphore_wait(barrier, 2 * len(STEPS) + len(LINE))

    started = []

    def send(src, dst, ssem, rsem, target):
        copy = pltpu.make_async_remote_copy(
            src_ref=src, dst_ref=dst, send_sem=ssem, recv_sem=rsem, device_id=target, device_id_type=MESH
        )
        copy.start()
        started.append(copy)
        return copy

    local = []

    def keep(src, dst, sem):
        copy = pltpu.make_async_copy(src, dst, sem)
        copy.start()
        local.append(copy)
        return copy

    mine = (z, y)
    halves = (pl.ds(0, WIDTHS[0]), pl.ds(*WIDTHS))

    def at(h, first, second):
        return (first, second) if h == 0 else (second, first)

    def first_step(h, step):
        return device(step, 0) if h == 0 else device(0, step)

    def second_step(h, step):
        return device(0, step) if h == 0 else device(step, 0)

    def pick(ref, h, first, second, *more):
        one, two = at(h, first, second)
        return ref.at[(one, two, *more)]

    every = slice(None)
    keep(cot_ref, cots.at[xc], own.at[0])
    keep(table_ref, tables.at[xc], own.at[1])
    a1 = [[None] * 3, [None] * 3]
    a2 = [[[None] * 3 for _ in range(4)] for _ in range(2)]
    for h in range(2):
        keep(rows_ref.at[z, y, :, :, halves[h]], relay_a[h].at[mine[h], mine[1 - h]], own.at[2 + h])
    for i, off in enumerate(LINE):
        tab = send(table_ref, tables.at[xc], tab_s.at[i], tab_r.at[i], device(0, 0, *off))
    tab_copies = started[-len(LINE) :]
    tail = cot_ref.shape[0] // 2
    parts = (pl.ds(0, tail), pl.ds(tail, tail))

    def send_cot(src, dst, k, target):
        return send(src, dst, cot_s.at[k], cot_r.at[k], target)

    near = [send_cot(cot_ref, cots.at[xc], i, device(0, 0, step)) for i, step in enumerate((1, 3))]
    for i, step in enumerate(STEPS):
        for h in range(2):
            to = (mine[h] + step) % 4
            a1[h][i] = send(
                pick(rows_ref, h, to, every, every, every, halves[h]),
                relay_a[h].at[mine[h]],
                a1_s.at[h, i],
                a1_r.at[h, i],
                first_step(h, step),
            )
    other_core = [send_cot(cot_ref, cots.at[xc], 4, device(0, 0, 0, 1))]

    def forward_rows(h, i, source):
        for j, step in enumerate(STEPS):
            to = (mine[1 - h] + step) % 4
            if source is None:
                src = pick(rows_ref, h, mine[h], to, every, every, halves[h])
                place = mine[h]
            else:
                src = relay_a[h].at[source, to]
                place = source
            a2[h][i][j] = send(src, held_a[h].at[mine[1 - h], place], a2_s.at[h, i, j], a2_r.at[h, i, j], second_step(h, step))

    for h in range(2):
        forward_rows(h, 3, None)

    def forward_a1(i):
        for h in range(2):
            a1[h][i].wait_recv()
            forward_rows(h, i, (mine[h] - STEPS[i]) % 4)

    line_copies, own_lines = ([], []), ([], [])

    def spread_rows(h, group, source, place):
        where = pick(rows_out, h, every, place, xc, every, halves[h])
        for k, off in enumerate(LINE):
            ox, oc = (x + off[0]) % 4, (c + off[1]) % 2
            line_copies[h].append(send(
                source.at[:, (ox % 2) * 2 + oc],
                where,
                a3_s.at[h, group, k],
                a3_r.at[h, group, k],
                device(0, 0, *off),
            ))
        own_lines[h].append(keep(source.at[:, sub], where, own.at[4 + 4 * h + group]))

    row = iota((16 * MROWS, 1), 0)

    def make_block(b):
        set_ends(rest, cots.at[b])
        choices = [(tables[b, k : k + 1, :], tables[b, 4 + k : 5 + k, :]) for k in range(4)]
        place_into(block_buf, (row // MROWS) * 4 + sub, row % MROWS, choices, cots.at[b], rest)
        sent[:, :, b] = block_buf[...].reshape(4, 4, MROWS, MAIN)

    b1 = [[[None] * 3, [None] * 3] for _ in range(4)]
    b2 = [[[[None] * 3 for _ in range(4)] for _ in range(2)] for _ in range(4)]

    def blocks_of(p):
        return pl.ds(((x - (0, 1, 3, 2)[p]) % 4) * 2, 2)

    def forward_wts(p, h, i, source):
        blocks = blocks_of(p)
        for j, step in enumerate(STEPS + (0,)):
            to = (mine[1 - h] + step) % 4
            if source is None:
                src = pick(sent, h, mine[h], to, blocks, every, halves[h])
                place = mine[h]
            else:
                src = relay_b[h].at[source, to, blocks]
                place = source
            dst = pick(wt_out, h, place, mine[1 - h], blocks, every, halves[h])
            if step:
                b2[p][h][i][j] = send(src, dst, b2_s.at[p, h, i, j], b2_r.at[p, h, i, j], second_step(h, step))
            else:
                keep(src, dst, own.at[12 + (p * 2 + h) * 4 + i])

    def send_part(p):
        start = ((x - (0, 1, 3, 2)[p]) % 4) * 2

        @pl.loop(0, 2)
        def _(b):
            make_block(start + b)

        for i, step in enumerate(STEPS):
            for h in range(2):
                to = (mine[h] + step) % 4
                b1[p][h][i] = send(
                    pick(sent, h, to, every, blocks_of(p), every, halves[h]),
                    relay_b[h].at[mine[h], :, blocks_of(p)],
                    b1_s.at[p, h, i],
                    b1_r.at[p, h, i],
                    first_step(h, step),
                )
        for h in range(2):
            forward_wts(p, h, 3, None)

    def relay_part(p):
        for i, step in enumerate(STEPS):
            for h in range(2):
                b1[p][h][i].wait_recv()
                forward_wts(p, h, i, (mine[h] - step) % 4)

    for copy in local[:4]:
        copy.wait()
    for copy in tab_copies:
        copy.wait_recv()
    other_core[0].wait_recv()
    if EARLY:
        send_part(0)
    forward_a1(0)
    forward_a1(1)
    weights = [pltpu.make_async_copy(gate_hbm, gate_w, own.at[44]), pltpu.make_async_copy(up_hbm, up_w, own.at[45])]
    for copy in weights:
        copy.start()
    far = []
    for i, step in enumerate((1, 3)):
        block = ((x - step) % 4) * 2 + c
        near[i].wait_recv()
        far.append(send_cot(cots.at[block, parts[i]], cots.at[block, parts[i]], 2 + i, device(0, 0, step)))
        other_core.append(send_cot(cots.at[block], cots.at[block], 5 + i, device(0, 0, 0, 1)))
    forward_a1(2)
    for h in range(2):
        spread_rows(h, 3, relay_a[h].at[:, mine[1 - h]], mine[1 - h])
    if not EARLY:
        send_part(0)
    for p in (1, 2):
        other_core[p].wait_recv()
        send_part(p)
    block = ((x + 2) % 4) * 2 + c
    for i in range(2):
        far[i].wait_recv()
        other_core.append(send_cot(cots.at[block, parts[i]], cots.at[block, parts[i]], 7 + i, device(0, 0, 0, 1)))
    for copy in other_core[3:]:
        copy.wait_recv()
    send_part(3)
    if EARLY:
        relay_part(0)
    for h in range(2):
        for j, step in enumerate(STEPS):
            for i in range(4):
                a2[h][i][j].wait_recv()
            place = (mine[1 - h] - step) % 4
            spread_rows(h, j, held_a[h].at[place], place)
    for p in range(1 if EARLY else 0, 4):
        relay_part(p)

    flat = rows_out.reshape(16 * 8 * MROWS, MAIN)
    for copy in weights:
        copy.wait()
    cut = WIDTHS[0]
    for copy in own_lines[0]:
        copy.wait()
    for copy in line_copies[0]:
        copy.wait_recv()
    unpack(flat, full_rows, 0, cut)
    glu[...] = dot_nt(full_rows[:, :cut], gate_w[:, :cut])
    slope[...] = dot_nt(full_rows[:, :cut], up_w[:, :cut])
    for copy in own_lines[1]:
        copy.wait()
    for copy in line_copies[1]:
        copy.wait_recv()
    unpack(flat, full_rows, cut, MAIN)
    keep(full_rows, full_out, own.at[46])
    glu[...] += dot_nt(full_rows[:, cut:], gate_w[:, cut:])
    slope[...] += dot_nt(full_rows[:, cut:], up_w[:, cut:])

    @pl.loop(0, full_rows.shape[0] // TILE)
    def _(i):
        tile = tile_of(i, TILE)
        gate, up = glu[tile, :], slope[tile, :] + 1.0
        sig = jax.nn.sigmoid(ALPHA * gate)
        prod = gate * sig
        hidden[tile, :] = (up * prod).astype(BF)
        glu[tile, :] = prod
        slope[tile, :] = up * (sig + ALPHA * prod * (1.0 - sig))

    for i, (src, dst) in enumerate(((hidden, hidden_out), (glu, glu_out), (slope, slope_out))):
        keep(src, dst, own.at[47 + i])
    early = {id(copy) for copy in tab_copies + near + far + other_core}
    for group in a1 + [v for half in a2 for v in half] + [v for part in b1 for v in part]:
        early |= {id(copy) for copy in group}
    for half in line_copies + own_lines:
        early |= {id(copy) for copy in half}
    for copy in local[4:]:
        if id(copy) not in early:
            copy.wait()
    for copy in started:
        if id(copy) not in early:
            copy.wait_recv()
    for copy in started:
        copy.wait_send()


def exchange(table, rows_msg, cot_t, gate_w, up_w):
    out = jax.ShapeDtypeStruct((4, 4, 8, MROWS, MAIN), BF)
    units, width = gate_w.shape
    rows = 16 * 8 * CAP
    anywhere = pl.BlockSpec(memory_space=pl.ANY)
    shapes = [(7,), (9,), (2, 3), (2, 4, 3), (2, 4, 7), (PARTS, 2, 3), (PARTS, 2, 4, 3)]
    sems = [pltpu.SemaphoreType.DMA(shape) for shape in shapes for _ in range(2)]
    return pl.pallas_call(
        exchange_kernel,
        in_specs=[anywhere] * 5,
        out_specs=[anywhere] * 5,
        out_shape=[
            out,
            jax.ShapeDtypeStruct((rows, width), BF),
            jax.ShapeDtypeStruct((rows, units), BF),
            jax.ShapeDtypeStruct((rows, units), F32),
            jax.ShapeDtypeStruct((rows, units), F32),
        ],
        scratch_shapes=[
            *[pltpu.VMEM((4, 4, at, MROWS, half), BF) for at in (4, 4, 8) for half in WIDTHS],
            pltpu.VMEM((8, *cot_t.shape), BF),
            pltpu.VMEM((8, *table.shape), F32),
            pltpu.VMEM((4, 4, 8, MROWS, MAIN), BF),
            pltpu.VMEM((MAIN - 3 * CHUNK, 3 * cot_t.shape[1]), BF),
            pltpu.VMEM((16 * MROWS, MAIN), BF),
            pltpu.VMEM((4, 4, 8, MROWS, MAIN), BF),
            pltpu.VMEM((units, width), BF),
            pltpu.VMEM((units, width), BF),
            pltpu.VMEM((rows, width), BF),
            pltpu.VMEM((rows, units), BF),
            pltpu.VMEM((rows, units), F32),
            pltpu.VMEM((rows, units), F32),
            *sems,
            pltpu.SemaphoreType.DMA((50,)),
        ],
        compiler_params=pltpu.CompilerParams(collective_id=0, has_side_effects=True, vmem_limit_bytes=67_043_328),
    )(table, rows_msg.reshape(4, 4, 4, MROWS, MAIN), cot_t, gate_w, up_w)


def expert_kernel(wt_msg, hidden_hbm, glu_hbm, slope_hbm, gate_hbm, up_hbm, down_hbm, *refs):
    outs, bufs, sems = refs[:4], refs[4:-2], refs[-2:]
    msg_wt, hidden, glu, slope, gate_w, up_w, down_w, weighted, gate_grad, up_grad, full, shares = bufs
    weighted_out, gate_grad_out, up_grad_out, packed_out = outs
    arrive, leave = sems
    total, width = weighted.shape
    tiles = total // TILE
    fetched = []
    for src, dst in (
        (wt_msg, msg_wt), (down_hbm, down_w), (hidden_hbm, hidden), (glu_hbm, glu), (slope_hbm, slope), (gate_hbm, gate_w), (up_hbm, up_w)
    ):
        fetched.append(pltpu.make_async_copy(src, dst, arrive.at[len(fetched)]))
        fetched[-1].start()
    puts = []

    def put(i, src, dst):
        copy = pltpu.make_async_copy(src, dst, leave.at[i])
        copy.start()
        return copy

    fetched[0].wait()
    unpack(msg_wt, weighted, 0, MAIN)
    puts.append(put(2, weighted, weighted_out))
    for copy in fetched[1:5]:
        copy.wait()
    main_t, rem_t, last_t = picks(WIDE, TILE, True, True)
    lane = iota((TILE, 128), 1)
    slot = iota((TILE, 128), 0) % CAP
    which = slot % 3
    spot = ENDS + 2 * which
    hgrad = dot_nt(weighted[...], down_w[...])
    share = jnp.sum(hgrad * hidden[...].astype(F32), axis=1, keepdims=True)
    up_grad[...] = (hgrad * glu[...]).astype(BF)
    gate_grad[...] = (hgrad * slope[...]).astype(BF)
    puts.append(put(3, gate_grad, gate_grad_out))
    puts.append(put(4, up_grad, up_grad_out))
    for copy in fetched[5:]:
        copy.wait()
    full[:, width:] = jnp.zeros((total, full.shape[1] - width), BF)
    for start in range(0, width, 768):
        cols = slice(start, min(width, start + 768))
        full[:, cols] = (dot(gate_grad[...], gate_w[:, cols]) + dot(up_grad[...], up_w[:, cols])).astype(BF)
    shares[...] = jnp.broadcast_to(share, shares.shape)

    @pl.loop(0, tiles)
    def _(i):
        tile, wide = tile_of(i, TILE), tile_of(i, WIDE)
        for j in range(3):
            cols = slice(j * CHUNK, (j + 1) * CHUNK)
            msg_wt[wide, cols] = (dot(main_t, full[tile, cols]) + dot(rem_t[j], full[tile, BODY])).astype(BF)
        part = shares[tile, :]
        head = part.astype(BF).astype(F32)
        pair = jnp.where(lane == spot, head, jnp.where(lane == spot + 1, part - head, 0.0))
        ends = full[tile, MAIN + CHUNK :].astype(F32)
        one = jnp.where(which == 0, ends, jnp.where(which == 1, pltpu.roll(ends, ENDS, 1), 0.0))
        two = jnp.where(which == 2, ends, 0.0) + pair
        for k, value in enumerate((one, two)):
            cols = slice(3 * CHUNK + 128 * k, 3 * CHUNK + 128 * (k + 1))
            msg_wt[wide, cols] = (dot(main_t, full[tile, cols]) + dot(last_t, value.astype(BF))).astype(BF)
        put(5 + i, msg_wt.at[wide], packed_out.at[wide])

    @pl.loop(0, tiles)
    def _(i):
        wide = tile_of(i, WIDE)
        pltpu.make_async_copy(msg_wt.at[wide], packed_out.at[wide], leave.at[5 + i]).wait()

    for copy in puts:
        copy.wait()


def expert(wt_msg, hidden, glu, slope, gate_w, up_w, down_w):
    units, width = gate_w.shape
    rows = hidden.shape[0]
    anywhere = pl.BlockSpec(memory_space=pl.ANY)
    wide, thin = (rows, width), (rows, units)
    return pl.pallas_call(
        expert_kernel,
        in_specs=[anywhere] * 7,
        out_specs=[anywhere] * 4,
        out_shape=[jax.ShapeDtypeStruct(shape, BF) for shape in (wide, thin, thin, wt_msg.shape)],
        scratch_shapes=[
            pltpu.VMEM(wt_msg.shape, BF),
            pltpu.VMEM(thin, BF),
            *[pltpu.VMEM(thin, F32)] * 2,
            *[pltpu.VMEM((units, width), BF)] * 3,
            pltpu.VMEM(wide, BF),
            *[pltpu.VMEM(thin, BF)] * 2,
            pltpu.VMEM((rows, MAIN + CHUNK + 128), BF),
            pltpu.VMEM((rows, 128), F32),
            pltpu.SemaphoreType.DMA((7,)),
            pltpu.SemaphoreType.DMA((5 + rows // TILE,)),
        ],
        compiler_params=pltpu.CompilerParams(vmem_limit_bytes=62 * 2**20),
        cost_estimate=pl.CostEstimate(flops=6 * rows * width * units, bytes_accessed=40 * 2**20, transcendentals=0),
    )(wt_msg, hidden, glu, slope, gate_w, up_w, down_w)


def combine_kernel(copies, expert_ref, slot_ref, slot_t_ref, prob_t_ref, back_hbm, in_ref, prob_out_ref, back_ref, sem):
    arrive = pltpu.make_async_copy(back_hbm, back_ref, sem)
    arrive.start()
    toks = in_ref.shape[0]
    total = back_ref.shape[0]
    col = iota((toks, total), 1)
    message = col // MROWS
    place = col - message * MROWS
    holder = message // copies
    zero = jnp.zeros((toks, total), F32)
    main, rem = zero, [zero] * 3
    sums = []
    lane = iota((toks, 128), 1)
    for k in range(expert_ref.shape[1]):
        expert, slot = expert_ref[:, k : k + 1], slot_ref[:, k : k + 1]
        kept = slot >= 0
        mine = holder == jnp.where(kept, expert, -1)
        high = jnp.where(slot >= 3, 1, 0)
        which = slot - 3 * high
        main = jnp.where(mine & (place == slot), 1.0, main)
        tail = mine & (place == CAP + high)
        for j in range(3):
            rem[j] = jnp.where(tail & (which == j), 1.0, rem[j])
        sums.append((jnp.where(tail, 1.0, 0.0).astype(BF), ENDS + 2 * which))
    main = main.astype(BF)
    rem = [value.astype(BF) for value in rem]
    arrive.wait()
    first, shares = back_ref[:, 3 * CHUNK : 3 * CHUNK + 128], back_ref[:, 3 * CHUNK + 128 :]
    in_ref[:, :MAIN] = dot(main, back_ref[...]).astype(BF)
    part = dot(rem[0], back_ref[:, :CHUNK])
    for j in (1, 2):
        part = part + dot(rem[j], back_ref[:, j * CHUNK : (j + 1) * CHUNK])
    in_ref[:, BODY] = part.astype(BF)
    ends = dot(rem[0], first) + pltpu.roll(dot(rem[1], first), ENDS, 1) + dot(rem[2], shares)
    in_ref[:, MAIN + CHUNK :] = ends[:, :ENDS].astype(BF)
    total_share = jnp.zeros((toks, 128), F32)
    for k, (tail, spot) in enumerate(sums):
        got = dot(tail, shares)
        got = jnp.where((lane == spot) | (lane == spot + 1), got, 0.0)
        total_share = jnp.where(lane == k, jnp.sum(got, axis=1, keepdims=True), total_share)
    share_t = total_share.T[: prob_out_ref.shape[0], :]
    rounded = prob_t_ref[...].astype(BF).astype(F32)
    prob_out_ref[...] = jnp.where(slot_t_ref[...] >= 0, share_t / rounded, 0.0)


def combine(expert_ids, slots, probs, back, width, copies):
    return pl.pallas_call(
        functools.partial(combine_kernel, copies),
        out_shape=(
            jax.ShapeDtypeStruct((expert_ids.shape[0], width), BF),
            jax.ShapeDtypeStruct(probs.T.shape, F32),
        ),
        in_specs=[*[pl.BlockSpec(memory_space=pltpu.VMEM)] * 4, pl.BlockSpec(memory_space=pl.ANY)],
        scratch_shapes=[pltpu.VMEM(back.shape, BF), pltpu.SemaphoreType.DMA],
        compiler_params=pltpu.CompilerParams(vmem_limit_bytes=40 * 2**20),
    )(expert_ids, slots, slots.T, probs.T, back)


def body(tokens, cotangent, expert_ids, slots, probs, w_gate, w_up, w_down):
    experts = lax.axis_size("expert")
    copies = lax.axis_size("dp")
    devices = experts * copies
    width = tokens.shape[1]
    gate_w, up_w, down_w = w_gate[0].T, w_up[0].T, w_down[0].T
    rows_msg, table = pack(expert_ids.T, slots.T, probs.T, tokens.T, experts)
    wt_in, rows, hidden, glu, slope = exchange(table, rows_msg, cotangent.T, gate_w, up_w)
    wt_in = wt_in.reshape(devices * MROWS, MAIN)
    weighted, gate_grad, up_grad, packed = expert(wt_in, hidden, glu, slope, gate_w, up_w, down_w)
    back = lax.all_to_all(
        packed.reshape(devices, MROWS, MAIN), ("expert", "dp"), split_axis=0, concat_axis=0, tiled=True
    ).reshape(devices * MROWS, MAIN)
    contract_rows = (((0,), (0,)), ((), ()))
    grad_down = lax.dot_general(weighted, hidden, contract_rows, preferred_element_type=F32).astype(BF)
    grad_gate = lax.dot_general(rows, gate_grad, contract_rows, preferred_element_type=F32).astype(BF)
    grad_up = lax.dot_general(rows, up_grad, contract_rows, preferred_element_type=F32).astype(BF)
    input_grad, prob_grad = combine(expert_ids, slots, probs, back, width, copies)
    return input_grad, prob_grad.T, grad_gate[None], grad_up[None], grad_down[None]


def solution(mesh):
    token_spec = P(("expert", "dp"), None)
    weight_spec = P("expert", None, "dp")
    return jax.shard_map(
        body,
        mesh=mesh,
        in_specs=(token_spec,) * 5 + (weight_spec,) * 3,
        out_specs=(token_spec,) * 2 + (weight_spec,) * 3,
        check_vma=False,
    )
```
